32 devices in a mesh: gx: 4 (over y, x), gy: 2 (over core), gz: 4 (over z).
Axes of the slice: x: 2, y: 2, z: 4, core: 2. Of those that a mesh axis runs over, the one named last changes fastest.
Arguments:
- residual_start: float32 [8, 4, 8, 81, 128], P('gx', 'gy', 'gz'), may hold values from -6 to 6
- patch_inverse: bfloat16 [8, 4, 8, 540, 540], P('gx', 'gy', 'gz'), may hold values from -0.05 to 0.4
- patch_order: int32 [8, 4, 8, 540], P('gx', 'gy', 'gz'), may hold values from 0 to 539, each once within a row
- element_matrix: float32 [8, 4, 8, 108, 108], P('gx', 'gy', 'gz'), may hold values from -1.6 to 6.5
- face_order: int32 [8, 4, 8, 6, 9], P('gx', 'gy', 'gz'), may hold values from 0 to 8, each once within a row
Outputs:
- solution: float32 [8, 4, 8, 81, 128], P('gx', 'gy', 'gz')
- residual: float32 [8, 4, 8, 81, 128], P('gx', 'gy', 'gz')
The draws below stay inside these ranges and needn't reach their ends.
Inputs may be any that keep to these rules, and one draw needn't show every extreme that they name: `patch_order`: each row lists each of the 540 canonical rows of a star once. `face_order`: each face's row lists each of its 9 degrees of freedom once.
All inputs are finite; a program needn't handle non-finite values.
Results may differ from the reference program's by a relative error of at most 0.0068.
Values may be sent and summed in bfloat16 or wider, within the bound.
No kernel may reach another device: no remote copies, remote signals or barrier semaphores. Data moves between devices by JAX's collectives and lax.ppermute only.
A program may use at most 128 MiB of HBM per device.

```python
import math
import jax
import jax.numpy as jnp
from jax import lax

RHS = 128
INNER = 54
FACE = 9
SWEEPS = 2
OWN = 81
LOCAL = 108
PATCH = 540
EX = 8
EY = 4
EZ = 8


def draw_patch_inverse(key, part):
    first, second = jax.random.split(jax.random.fold_in(key, 11), 2)
    shape = (EX, EY, EZ, PATCH, PATCH)
    noise = jnp.clip(jax.random.normal(first, shape, jnp.float32), -4.0, 4.0) * (0.4 / math.sqrt(PATCH))
    diagonal = jax.random.uniform(second, (EX, EY, EZ, PATCH, 1), jnp.float32, 0.6, 1.4)
    eye = (jnp.arange(PATCH)[:, None] == jnp.arange(PATCH)[None, :]).astype(jnp.float32)
    matrix = noise + diagonal * eye
    return (0.125 * matrix).astype(jnp.bfloat16)


def draw_element_matrix(key, part):
    first, second, third = jax.random.split(jax.random.fold_in(key, 23), 3)
    shape = (EX, EY, EZ, LOCAL, LOCAL)
    noise = jnp.clip(jax.random.normal(first, shape, jnp.float32), -4.0, 4.0) * (0.4 / math.sqrt(LOCAL))
    diagonal = jax.random.uniform(second, (EX, EY, EZ, LOCAL, 1), jnp.float32, 0.8, 1.2)
    eye = (jnp.arange(LOCAL)[:, None] == jnp.arange(LOCAL)[None, :]).astype(jnp.float32)
    low, high = (math.log(0.5), math.log(2.0))
    coefficient = jnp.exp(jax.random.uniform(third, (EX, EY, EZ, 1, 1), jnp.float32, low, high))
    return coefficient * (noise + diagonal * eye)


def steps_of(key, dims, shards, least, high):
    loudness = 1.0
    for dim, blocks in shards:
        draws = jax.random.uniform(jax.random.fold_in(jax.random.fold_in(key, 6), dim), (blocks,), jnp.float32, least / len(shards), high / len(shards))
        loudness = loudness * jnp.repeat(jnp.exp(draws), dims[dim] // blocks).reshape((-1,) + (1,) * (len(dims) - 1 - dim))
    return loudness


def bell_draw(stream_key, extent, deviation, most, cuts=(), kind=jnp.bfloat16):
    array = jax.random.normal(stream_key, extent, jnp.float32) * deviation
    if len(cuts) > 0:
        array = steps_of(stream_key, extent, cuts, -0.22, 0.18) * array
    return jnp.clip(array, min=-most, max=most).astype(kind)


def setup_inputs(seed: int = 0) -> dict:
    splits = jax.random.split(jax.random.key(seed), 6)
    residual_start = bell_draw(splits[0], (EX, EY, EZ, OWN, RHS), 1.0, 6.0, ((0, 4), (1, 2), (2, 4)), jnp.float32)
    patch_inverse = draw_patch_inverse(jax.random.fold_in(splits[5], 71), 0)
    patch_order = jax.vmap(lambda own: jax.random.permutation(own, PATCH))(jax.random.split(splits[2], EX * EY * EZ)).reshape((EX, EY, EZ, PATCH)).astype(jnp.int32)
    element_matrix = draw_element_matrix(jax.random.fold_in(splits[5], 71), 0)
    face_order = jax.vmap(lambda own: jax.random.permutation(own, FACE))(jax.random.split(splits[4], EX * EY * EZ * 6)).reshape((EX, EY, EZ, 6, FACE)).astype(jnp.int32)
    return {"residual_start": residual_start, "patch_inverse": patch_inverse, "patch_order": patch_order, "element_matrix": element_matrix, "face_order": face_order}


def face_mask(start_y, start_z, cells_y, cells_z):
    rows = jnp.arange(INNER + 3 * FACE, dtype=jnp.int32)
    in_second = (rows >= INNER + FACE) & (rows < INNER + 2 * FACE)
    in_third = rows >= INNER + 2 * FACE
    index_y = start_y + jnp.arange(cells_y, dtype=jnp.int32)
    index_z = start_z + jnp.arange(cells_z, dtype=jnp.int32)
    removed = (in_second[None, None, :] & (index_y == 0)[:, None, None]) | (in_third[None, None, :] & (index_z == 0)[None, :, None])
    return jnp.where(removed, 0.0, 1.0).astype(jnp.float32)[None, :, :, :, None]


def star_vectors(extended, counts):
    cells_x, cells_y, cells_z = counts
    pieces = []
    for xoffset in (0, 1):
        for yoffset in (0, 1):
            for zoffset in (0, 1):
                pieces.append(extended[xoffset:xoffset + cells_x, yoffset:yoffset + cells_y, zoffset:zoffset + cells_z, :INNER])
    for first in (0, 1):
        for second in (0, 1):
            pieces.append(extended[1:1 + cells_x, first:first + cells_y, second:second + cells_z, INNER:INNER + FACE])
    for first in (0, 1):
        for second in (0, 1):
            pieces.append(extended[first:first + cells_x, 1:1 + cells_y, second:second + cells_z, INNER + FACE:INNER + 2 * FACE])
    for first in (0, 1):
        for second in (0, 1):
            pieces.append(extended[first:first + cells_x, second:second + cells_y, 1:1 + cells_z, INNER + 2 * FACE:])
    return jnp.concatenate(pieces, axis=3)


def place_corrections(solved, counts):
    total = None
    face_base = 8 * INNER
    for xoffset in (0, 1):
        for yoffset in (0, 1):
            for zoffset in (0, 1):
                member = 4 * xoffset + 2 * yoffset + zoffset
                parts = [solved[..., INNER * member:INNER * (member + 1), :]]
                blank = jnp.zeros(solved.shape[:3] + (FACE, solved.shape[4]), jnp.float32)
                start = face_base + FACE * (2 * yoffset + zoffset)
                parts.append(solved[..., start:start + FACE, :] if xoffset == 1 else blank)
                start = face_base + 4 * FACE + FACE * (2 * xoffset + zoffset)
                parts.append(solved[..., start:start + FACE, :] if yoffset == 1 else blank)
                start = face_base + 8 * FACE + FACE * (2 * xoffset + yoffset)
                parts.append(solved[..., start:start + FACE, :] if zoffset == 1 else blank)
                block = jnp.concatenate(parts, axis=3)
                block = jnp.pad(block, ((xoffset, 1 - xoffset), (yoffset, 1 - yoffset), (zoffset, 1 - zoffset), (0, 0), (0, 0)))
                total = block if total is None else total + block
    return total


def apply_patches(vectors, inverses, order):
    picked = jnp.take_along_axis(vectors, order[:, :, None], axis=1)
    solved = jnp.einsum('vts,vsr->vtr', inverses.astype(jnp.float32), picked.astype(jnp.float32))
    back = jnp.argsort(order, axis=1).astype(jnp.int32)
    return jnp.take_along_axis(solved, back[:, :, None], axis=1)


def element_change(owned, uppers, matrices, face_order):
    faces = [owned[..., INNER:INNER + FACE, :], uppers[0], owned[..., INNER + FACE:INNER + 2 * FACE, :], uppers[1], owned[..., INNER + 2 * FACE:, :], uppers[2]]
    stacked = jnp.stack(faces, axis=3)
    onehot = (face_order[..., None] == jnp.arange(FACE, dtype=jnp.int32)).astype(jnp.float32)
    high = lax.Precision.HIGHEST
    local_faces = jnp.einsum('xyzfst,xyzftr->xyzfsr', onehot, stacked, precision=high)
    shape = owned.shape
    local = jnp.concatenate([owned[..., :INNER, :], local_faces.reshape(shape[:3] + (6 * FACE, shape[4]))], axis=3)
    image = jnp.einsum('xyzij,xyzjr->xyzir', matrices, local, precision=high)
    image_faces = image[..., INNER:, :].reshape(shape[:3] + (6, FACE, shape[4]))
    out_faces = jnp.einsum('xyzfst,xyzfsr->xyzftr', onehot, image_faces, precision=high)
    own_change = jnp.concatenate([image[..., :INNER, :], out_faces[:, :, :, 0], out_faces[:, :, :, 2], out_faces[:, :, :, 4]], axis=3)
    return own_change, (out_faces[:, :, :, 1], out_faces[:, :, :, 3], out_faces[:, :, :, 5])


def reference(residual_start, patch_inverse, patch_order, element_matrix, face_order):
    mask = face_mask(0, 0, EY, EZ)
    residual = residual_start * mask
    solution = jnp.zeros_like(residual)
    columns = residual.shape[4]
    for repeat in range(SWEEPS):
        rounded = residual.astype(jnp.bfloat16)
        extended = jnp.concatenate([rounded[-1:], rounded], axis=0)
        extended = jnp.pad(extended, ((0, 0), (1, 0), (1, 0), (0, 0), (0, 0)))

        def slab(carry, index):
            window = lax.dynamic_slice_in_dim(extended, index, 2, 0)
            vectors = star_vectors(window, (1, EY, EZ)).reshape(EY * EZ, PATCH, columns)
            inverses = lax.dynamic_index_in_dim(patch_inverse, index, 0, keepdims=False).reshape(EY * EZ, PATCH, PATCH)
            order = lax.dynamic_index_in_dim(patch_order, index, 0, keepdims=False).reshape(EY * EZ, PATCH)
            solved = apply_patches(vectors, inverses, order).reshape(1, EY, EZ, PATCH, columns)
            block = place_corrections(solved, (1, EY, EZ))
            current = lax.dynamic_slice_in_dim(carry, index, 2, 0)
            return lax.dynamic_update_slice_in_dim(carry, current + block, index, 0), None

        start = jnp.zeros((EX + 1, EY + 1, EZ + 1, OWN, columns), jnp.float32)
        total, unused = lax.scan(slab, start, jnp.arange(EX, dtype=jnp.int32))
        inside = total[:, 1:, 1:]
        owned = inside[1:]
        owned = jnp.concatenate([owned[:-1], owned[-1:] + inside[:1]], axis=0) * mask
        solution = solution + owned
        blank_y = jnp.zeros_like(owned[:, :1, :, :FACE])
        blank_z = jnp.zeros_like(owned[:, :, :1, :FACE])
        upper_x = jnp.roll(owned[..., INNER:INNER + FACE, :], -1, axis=0)
        upper_y = jnp.concatenate([owned[:, 1:, :, INNER + FACE:INNER + 2 * FACE], blank_y], axis=1)
        upper_z = jnp.concatenate([owned[:, :, 1:, INNER + 2 * FACE:], blank_z], axis=2)
        own_change, terms = element_change(owned, (upper_x, upper_y, upper_z), element_matrix, face_order)
        moved_x = jnp.roll(terms[0], 1, axis=0)
        moved_y = jnp.concatenate([blank_y, terms[1][:, :-1]], axis=1)
        moved_z = jnp.concatenate([blank_z, terms[2][:, :, :-1]], axis=2)
        extra = jnp.concatenate([jnp.zeros_like(owned[..., :INNER, :]), moved_x, moved_y, moved_z], axis=3)
        residual = residual - (own_change + extra) * mask
    return solution, residual
```

```python
import functools
import itertools

import jax
import jax.numpy as jnp
import numpy as np
from jax import lax
from jax.experimental import pallas as pl
from jax.experimental.pallas import tpu as pltpu
from jax.sharding import PartitionSpec as P

INNER = 54
FACE = 9
OWN = INNER + 3 * FACE
LOCAL = INNER + 6 * FACE
SWEEPS = 2
PATCH = 540
SLOT = 96
WIDE = 8 * SLOT
AXES = ("gx", "gy", "gz")
CORNERS = tuple(itertools.product((0, 1), repeat=3))
X0, Y0, Z0 = INNER, INNER + FACE, INNER + 2 * FACE
f32, bf16 = jnp.float32, jnp.bfloat16
VMEM_LIMIT = 12 * 1024 * 1024


def wide_rows():
    rows = np.full((WIDE,), -1, np.int32)
    for a, b, c in CORNERS:
        m = 4 * a + 2 * b + c
        base = m * SLOT
        rows[base : base + INNER] = INNER * m + np.arange(INNER)
        starts = (2 * b + c, 4 + 2 * a + c, 8 + 2 * a + b)
        for d, face in enumerate(starts):
            low = base + INNER + d * FACE
            rows[low : low + FACE] = 8 * INNER + face * FACE + np.arange(FACE)
    return np.ascontiguousarray(np.broadcast_to(rows[:, None], (WIDE, 128)))


def prepare_kernel(inv, order, rows, mat, slot, wide, canon):
    hot = jnp.where(rows[:, :1] == order[0], 1.0, 0.0).astype(bf16)
    half = lax.dot_general(inv[0], hot, (((1,), (1,)), ((), ())), preferred_element_type=f32)
    wide[0] = jnp.dot(hot, half.astype(bf16), preferred_element_type=f32).astype(bf16)
    high = lax.Precision.HIGHEST
    index = lax.broadcasted_iota(jnp.int32, (LOCAL, LOCAL), 0)
    pick = jnp.where(index == slot[0], 1.0, 0.0).astype(f32)
    side = lax.dot_general(
        mat[0], pick, (((1,), (1,)), ((), ())), precision=high, preferred_element_type=f32
    )
    canon[0] = jnp.dot(pick, side, precision=high, preferred_element_type=f32)


def prepare(inverse, order, matrices, face_order):
    count = inverse.shape[0]
    offsets = (INNER + FACE * jnp.arange(6, dtype=jnp.int32))[:, None]
    slots = (face_order + offsets).reshape(count, 1, 6 * FACE)
    inner = jnp.broadcast_to(jnp.arange(INNER, dtype=jnp.int32), (count, 1, INNER))
    slots = jnp.concatenate([inner, slots], axis=2)
    flops = count * 2 * WIDE * PATCH * (PATCH + WIDE)
    one = lambda i: (i, 0, 0)
    return pl.pallas_call(
        prepare_kernel,
        grid=(count,),
        in_specs=[
            pl.BlockSpec((1, PATCH, PATCH), one),
            pl.BlockSpec((1, 1, PATCH), one),
            pl.BlockSpec((WIDE, 128), lambda i: (0, 0)),
            pl.BlockSpec((1, LOCAL, LOCAL), one),
            pl.BlockSpec((1, 1, LOCAL), one),
        ],
        out_specs=[
            pl.BlockSpec((1, WIDE, WIDE), one),
            pl.BlockSpec((1, LOCAL, LOCAL), one),
        ],
        out_shape=[
            jax.ShapeDtypeStruct((count, WIDE, WIDE), bf16),
            jax.ShapeDtypeStruct((count, LOCAL, LOCAL), f32),
        ],
        compiler_params=pltpu.CompilerParams(vmem_limit_bytes=VMEM_LIMIT),
        cost_estimate=pl.CostEstimate(
            flops=flops, bytes_accessed=count * 2 * (PATCH * PATCH + WIDE * WIDE), transcendentals=0
        ),
        name="prepare",
    )(inverse, order, jnp.asarray(wide_rows()), matrices, slots)


def call(kernel, operands, shapes, name):
    specs = [pl.BlockSpec(memory_space=pltpu.SMEM)]
    specs += [pl.BlockSpec(memory_space=pltpu.VMEM)] * (len(operands) - 1)
    return pl.pallas_call(
        kernel,
        in_specs=specs,
        out_specs=[pl.BlockSpec(memory_space=pltpu.VMEM)] * len(shapes),
        out_shape=[jax.ShapeDtypeStruct(s, t) for s, t in shapes],
        compiler_params=pltpu.CompilerParams(vmem_limit_bytes=VMEM_LIMIT),
        name=name,
    )(*operands)


def cat(*parts):
    return jnp.concatenate(parts, axis=0)


def zeros(rows, like):
    return jnp.zeros((rows, like.shape[-1]), f32)


def start_kernel(cells, flags, res, out, my):
    cx, cy, cz = cells
    for x, y, z in itertools.product(*map(range, cells)):
        e = (x * cy + y) * cz + z
        cur = res[e]
        if y == 0:
            cur = cat(cur[:Y0], cur[Y0:Z0] * flags[0], cur[Z0:])
        if z == 0:
            cur = cat(cur[:Z0], cur[Z0:] * flags[2])
        out[e] = cur
        if y == cy - 1:
            nine, rest = zeros(FACE, cur), zeros(112 - OWN, cur)
            my[x * cz + z] = cat(cur[:Y0], nine, cur[Z0:], rest).astype(bf16)


def spread_kernel(cells, terms, *refs):
    cx, cy, cz = cells
    if terms:
        flags, res, yr, tx, tz, out, mx, mz, mxz = refs
    else:
        flags, res, yr, out, mx, mz, mxz = refs
    for x, z in itertools.product(range(cx), range(cz)):
        lastx, lastz = x == cx - 1, z == cz - 1
        halo = yr[0, x * cz + z].astype(f32) * flags[0]
        nine = zeros(FACE, halo)
        if lastx:
            mx[z] = cat(halo[:X0], halo[81:90], nine, halo[Z0:OWN]).astype(bf16)
        if lastz:
            mz[x * (cy + 1)] = cat(halo[:Y0], nine, halo[90:99]).astype(bf16)
        if lastx and lastz:
            mxz[0] = cat(halo[:X0], halo[81:90], nine, halo[90:99]).astype(bf16)
        for y in range(cy):
            e = (x * cy + y) * cz + z
            cur = res[e]
            if y == 0 and terms:
                cur = cat(cur[:Y0], cur[Y0:Z0] + halo[Y0:Z0], cur[Z0:])
            out[e] = cur
            upx = tx[y * cz + z][:FACE] if terms and lastx else nine
            upz = tz[x * cy + y][:FACE] if terms and lastz else nine
            if lastx:
                mx[(y + 1) * cz + z] = cat(cur[:X0], upx, cur[Y0:]).astype(bf16)
            if lastz:
                mz[x * (cy + 1) + y + 1] = cat(cur[:Z0], upz).astype(bf16)
            if lastx and lastz:
                mxz[y + 1] = cat(cur[:X0], upx, cur[Y0:Z0], upz).astype(bf16)


def solve_kernel(cells, flags, wide, res, yr, hx, hz, hxz, c, ox, oz, oxz, stars, solved):
    cx, cy, cz = cells
    step = pl.program_id(0)

    @pl.when(step == 0)
    def _():
        found = {}
        for e in itertools.product(range(-1, cx), range(-1, cy), range(-1, cz)):
            x, y, z = e
            if x < 0 and z < 0:
                val = hxz[y + 1].astype(f32)
            elif x < 0:
                val = hx[(y + 1) * cz + z].astype(f32)
            elif z < 0:
                val = hz[x * (cy + 1) + y + 1].astype(f32)
            elif y < 0:
                val = yr[0, x * cz + z].astype(f32)[:OWN] * flags[0]
            else:
                val = res[(x * cy + y) * cz + z]
            found[e] = val
        for n, v in enumerate(itertools.product(*map(range, cells))):
            for a, b, g in CORNERS:
                x, y, z = v[0] - 1 + a, v[1] - 1 + b, v[2] - 1 + g
                val = found[(x, y, z)]
                nine = zeros(FACE, val)
                part = cat(
                    val[:X0],
                    val[X0:Y0] if a or x < 0 else nine,
                    val[Y0:Z0] if b else nine,
                    val[Z0:] if g or z < 0 else nine,
                    zeros(SLOT - OWN, val),
                )
                m = 4 * a + 2 * b + g
                stars[n, m * SLOT : (m + 1) * SLOT] = part.astype(bf16)

    solved[step] = jnp.dot(wide[0], stars[step], preferred_element_type=f32)

    @pl.when(step == pl.num_programs(0) - 1)
    def _():
        vertices = list(itertools.product(*map(range, cells)))
        for e in itertools.product(range(-1, cx), range(-1, cy), range(-1, cz)):
            parts = []
            for n, v in enumerate(vertices):
                m = tuple(e[d] - v[d] + 1 for d in range(3))
                if all(k in (0, 1) for k in m):
                    parts.append((n, m))

            def total(low, high, keep):
                acc = None
                for n, m in parts:
                    if keep(m):
                        base = (4 * m[0] + 2 * m[1] + m[2]) * SLOT
                        val = solved[n, base + low : base + high]
                        acc = val if acc is None else acc + val
                return acc

            pieces = [total(0, X0, lambda m: True)]
            for d in range(3):
                low = INNER + d * FACE
                pieces.append(total(low, low + FACE, lambda m: e[d] < 0 or m[d] == 1))
            val = cat(*pieces)
            x, y, z = e
            if x < 0 and z < 0:
                oxz[y + 1] = val.astype(bf16)
            elif x < 0:
                ox[(y + 1) * cz + z] = val.astype(bf16)
            elif z < 0:
                oz[x * (cy + 1) + y + 1] = val.astype(bf16)
            else:
                c[(x * (cy + 1) + y + 1) * cz + z] = val


def solve(cells, flags, wide, res, yr, hx, hz, hxz):
    cx, cy, cz = cells
    count, columns = wide.shape[0], res.shape[-1]
    whole = lambda a: pl.BlockSpec(a.shape, lambda i, n=a.ndim: (0,) * n)
    shapes = [
        jax.ShapeDtypeStruct((cx * (cy + 1) * cz, OWN, columns), f32),
        jax.ShapeDtypeStruct(hx.shape, bf16),
        jax.ShapeDtypeStruct(hz.shape, bf16),
        jax.ShapeDtypeStruct(hxz.shape, bf16),
    ]
    return pl.pallas_call(
        functools.partial(solve_kernel, cells),
        grid=(count,),
        in_specs=[
            pl.BlockSpec(memory_space=pltpu.SMEM),
            pl.BlockSpec((1, WIDE, WIDE), lambda i: (i, 0, 0)),
        ]
        + [whole(a) for a in (res, yr, hx, hz, hxz)],
        out_specs=[whole(s) for s in shapes],
        out_shape=shapes,
        scratch_shapes=[
            pltpu.VMEM((count, WIDE, columns), bf16),
            pltpu.VMEM((count, WIDE, columns), f32),
        ],
        compiler_params=pltpu.CompilerParams(vmem_limit_bytes=VMEM_LIMIT),
        name="solve",
    )(flags, wide, res, yr, hx, hz, hxz)


def add_received(val, x, y, z, cells, gx, gz, gxz):
    cx, cy, cz = cells
    nine = zeros(FACE, val)
    if x == cx - 1:
        got = gx[(y + 1) * cz + z].astype(f32)
        val = val + cat(got[:X0], nine, got[Y0:])
    if z == cz - 1:
        got = gz[x * (cy + 1) + y + 1].astype(f32)
        val = val + cat(got[:Z0], nine)
    if x == cx - 1 and z == cz - 1:
        got = gxz[y + 1].astype(f32)
        val = val + cat(got[:X0], nine, got[Y0:Z0], nine)
    return val


def upper_x(y, z, cells, gx, gxz):
    val = gx[(y + 1) * cells[2] + z].astype(f32)[X0:Y0]
    if z == cells[2] - 1:
        val = val + gxz[y + 1].astype(f32)[X0:Y0]
    return val


def upper_z(x, y, cells, gz, gxz):
    val = gz[x * (cells[1] + 1) + y + 1].astype(f32)[Z0:]
    if x == cells[0] - 1:
        val = val + gxz[y + 1].astype(f32)[Z0:]
    return val


def reduce_kernel(cells, flags, c, gx, gz, gxz, out):
    cx, cy, cz = cells
    for x, z in itertools.product(range(cx), range(cz)):
        val = add_received(c[x * (cy + 1) * cz + z], x, -1, z, cells, gx, gz, gxz)
        nine = zeros(FACE, val)
        upx = upper_x(-1, z, cells, gx, gxz) if x == cx - 1 else nine
        upz = upper_z(x, -1, cells, gz, gxz) if z == cz - 1 else nine
        out[x * cz + z] = cat(val, upx, upz, zeros(104 - OWN - 2 * FACE, val))


def element_kernel(cells, first, last, *refs):
    cx, cy, cz = cells
    flags, c, gx, gz, gxz, yr, mat, res, hx, hz = refs[:10]
    refs = refs[10:]
    if not first:
        prev, refs = refs[0], refs[1:]
    sol, out, tx, tz, my = refs
    peer = yr.shape[0] - 1
    own, images = {}, {}
    for e in itertools.product(*map(range, cells)):
        x, y, z = e
        n = (x * cy + y) * cz + z
        val = add_received(c[(x * (cy + 1) + y + 1) * cz + z], x, y, z, cells, gx, gz, gxz)
        if y == cy - 1:
            got = yr[peer, x * cz + z][:OWN] * flags[1]
            val = val + cat(got[:Y0], zeros(FACE, val), got[Z0:])
        if y == 0:
            val = cat(val[:Y0], val[Y0:Z0] * flags[0], val[Z0:])
        if z == 0:
            val = cat(val[:Z0], val[Z0:] * flags[2])
        own[e] = val
        sol[n] = val if first else prev[n] + val
    for e in itertools.product(*map(range, cells)):
        x, y, z = e
        if x < cx - 1:
            upx = own[(x + 1, y, z)][X0:Y0]
        else:
            upx = upper_x(y, z, cells, gx, gxz)
            if y == cy - 1:
                upx = upx + yr[peer, x * cz + z][81:90] * flags[1]
        if y < cy - 1:
            upy = own[(x, y + 1, z)][Y0:Z0]
        else:
            upy = yr[peer, x * cz + z][Y0:Z0] * flags[1]
        if z < cz - 1:
            upz = own[(x, y, z + 1)][Z0:]
        else:
            upz = upper_z(x, y, cells, gz, gxz)
            if y == cy - 1:
                upz = upz + yr[peer, x * cz + z][90:99] * flags[1]
        val = own[e]
        local = cat(val[:Y0], upx, val[Y0:Z0], upy, val[Z0:], upz)
        images[e] = jnp.dot(
            mat[(x * cy + y) * cz + z],
            local,
            precision=lax.Precision.HIGHEST,
            preferred_element_type=f32,
        )
    for e in itertools.product(*map(range, cells)):
        x, y, z = e
        n = (x * cy + y) * cz + z
        old, image = res[n], images[e]
        lowx = old[X0:Y0] - image[54:63]
        lowy = old[Y0:Z0] - image[72:81]
        lowz = old[Z0:] - image[90:99]
        if x > 0:
            lowx = lowx - images[(x - 1, y, z)][63:72]
        else:
            lowx = lowx + hx[(y + 1) * cz + z].astype(f32)[X0:Y0]
        if y > 0:
            lowy = lowy - images[(x, y - 1, z)][81:90]
        else:
            lowy = lowy * flags[0]
        if z > 0:
            lowz = lowz - images[(x, y, z - 1)][99:108]
        else:
            lowz = (lowz + hz[x * (cy + 1) + y + 1].astype(f32)[Z0:]) * flags[2]
        val = cat(old[:X0] - image[:X0], lowx, lowy, lowz)
        out[n] = val
        nine, seven = zeros(FACE, val), zeros(16 - FACE, val)
        upx, upy, upz = -image[63:72], -image[81:90], -image[99:108]
        if x == cx - 1:
            tx[y * cz + z] = cat(upx, seven)
        if z == cz - 1:
            tz[x * cy + y] = cat(upz, seven)
        if y == cy - 1 and last:
            my[x * cz + z] = cat(upy, seven)
        elif y == cy - 1:
            my[x * cz + z] = cat(
                val[:Y0],
                upy,
                val[Z0:],
                upx if x == cx - 1 else nine,
                upz if z == cz - 1 else nine,
                zeros(112 - OWN - 2 * FACE, val),
            ).astype(bf16)


def finish_kernel(cells, flags, res, fx, fy, fz, out):
    cx, cy, cz = cells
    for x, y, z in itertools.product(*map(range, cells)):
        n = (x * cy + y) * cz + z
        cur = res[n]
        lowx, lowy, lowz = cur[X0:Y0], cur[Y0:Z0], cur[Z0:]
        if x == 0:
            lowx = lowx + fx[y * cz + z][:FACE]
        if y == 0:
            lowy = lowy + fy[0, x * cz + z][:FACE] * flags[0]
        if z == 0:
            lowz = lowz + fz[x * cy + y][:FACE]
        out[n] = cat(cur[:X0], lowx, lowy, lowz)


def route(offset):
    sizes = [lax.axis_size(a) for a in AXES]
    flat = lambda c: (c[0] * sizes[1] + c[1]) * sizes[2] + c[2]
    pairs = []
    for spot in itertools.product(*map(range, sizes)):
        aim = [s + o for s, o in zip(spot, offset)]
        aim[0] %= sizes[0]
        if all(0 <= a < s for a, s in zip(aim, sizes)):
            pairs.append((flat(spot), flat(aim)))
    return pairs


def send_xz(mx, mz, mxz, sign):
    return (
        lax.ppermute(mx, AXES, route((sign, 0, 0))),
        lax.ppermute(mz, AXES, route((0, 0, sign))),
        lax.ppermute(mxz, AXES, route((sign, 0, sign))),
    )


def send_y(my, sign):
    if lax.axis_size("gy") == 2:
        return lax.all_gather(my, "gy")
    return lax.ppermute(my, AXES, route((0, sign, 0)))[None]


def body(residual_start, patch_inverse, patch_order, element_matrix, face_order):
    cells = cx, cy, cz = residual_start.shape[:3]
    if min(cells) < 2:
        raise ValueError(cells)
    columns = residual_start.shape[4]
    count = cx * cy * cz
    at_y, at_z = lax.axis_index("gy"), lax.axis_index("gz")
    flags = jnp.stack([at_y > 0, at_y < lax.axis_size("gy") - 1, at_z > 0]).astype(f32)
    bind = lambda kernel, *extra: functools.partial(kernel, cells, *extra)
    state = ((count, OWN, columns), f32)
    sent = (
        (((cy + 1) * cz, OWN, columns), bf16),
        ((cx * (cy + 1), OWN, columns), bf16),
        ((cy + 1, OWN, columns), bf16),
    )
    term_x, term_y, term_z = (((n, 16, columns), f32) for n in (cy * cz, cx * cz, cx * cy))
    rim = ((cx * cz, 112, columns), bf16)

    start = residual_start.reshape(count, OWN, columns)
    residual, my = call(bind(start_kernel), [flags, start], [state, rim], "start")
    wide, canon = prepare(
        patch_inverse.reshape(count, PATCH, PATCH),
        patch_order.reshape(count, 1, PATCH),
        element_matrix.reshape(count, LOCAL, LOCAL),
        face_order,
    )
    terms, solution = [], []
    for sweep in range(SWEEPS):
        first, last = sweep == 0, sweep == SWEEPS - 1
        yr = send_y(my, 1)
        residual, mx, mz, mxz = call(
            bind(spread_kernel, not first), [flags, residual, yr] + terms, [state, *sent], "spread"
        )
        hx, hz, hxz = send_xz(mx, mz, mxz, 1)
        c, ox, oz, oxz = solve(cells, flags, wide, residual, yr, hx, hz, hxz)
        gx, gz, gxz = send_xz(ox, oz, oxz, -1)
        (down,) = call(
            bind(reduce_kernel), [flags, c, gx, gz, gxz], [((cx * cz, 104, columns), f32)], "reduce"
        )
        back = send_y(down, -1)
        total, residual, tx, tz, my = call(
            bind(element_kernel, first, last),
            [flags, c, gx, gz, gxz, back, canon, residual, hx, hz] + solution,
            [state, state, term_x, term_z, term_y if last else rim],
            "element",
        )
        terms, solution = [tx, tz], [total]
    fx = lax.ppermute(tx, AXES, route((1, 0, 0)))
    fz = lax.ppermute(tz, AXES, route((0, 0, 1)))
    fy = send_y(my, 1)
    (residual,) = call(bind(finish_kernel), [flags, residual, fx, fy, fz], [state], "finish")
    shape = residual_start.shape
    return total.reshape(shape), residual.reshape(shape)


def solution(mesh):
    return jax.shard_map(
        body,
        mesh=mesh,
        in_specs=(
            P("gx", "gy", "gz", None, None),
            P("gx", "gy", "gz", None, None),
            P("gx", "gy", "gz", None),
            P("gx", "gy", "gz", None, None),
            P("gx", "gy", "gz", None, None),
        ),
        out_specs=(P("gx", "gy", "gz", None, None), P("gx", "gy", "gz", None, None)),
        check_vma=False,
    )
```

```python
import functools
import itertools

import jax
import jax.numpy as jnp
from jax import lax
from jax.experimental import pallas as pl
from jax.experimental.pallas import tpu as pltpu
from jax.sharding import PartitionSpec as P

INNER = 54
FACE = 9
OWN = INNER + 3 * FACE
LOCAL = INNER + 6 * FACE
SWEEPS = 2
PATCH = 540
SLOT = 96
WIDE = 8 * SLOT
AXES = ("gx", "gy", "gz")
CORNERS = tuple(itertools.product((0, 1), repeat=3))
X0, Y0, Z0 = INNER, INNER + FACE, INNER + 2 * FACE
f32, bf16 = jnp.float32, jnp.bfloat16
VMEM_LIMIT = 12 * 1024 * 1024


def canonical_rows(q):
    m = (q * 683) >> 16
    r = q - SLOT * m
    d = ((r - INNER) * 57) >> 9
    a, b, c = m >> 2, (m >> 1) & 1, m & 1
    face = jnp.where(d == 0, 2 * b + c, jnp.where(d == 1, 4 + 2 * a + c, 8 + 2 * a + b))
    on_face = 8 * INNER + FACE * face + r - INNER - FACE * d
    row = jnp.where(r < INNER, INNER * m + r, jnp.where(r < OWN, on_face, -1))
    return row.astype(f32)


def tables_kernel(cells, inv, order, matrix, pick, back, loaded, sems):
    cx, cy, cz = cells
    copies = [
        pltpu.make_async_copy(inv.at[n // cy, n % cy], loaded.at[n], sems.at[n])
        for n in range(cx * cy)
    ]
    for copy in copies:
        copy.start()
    across = canonical_rows(lax.broadcasted_iota(jnp.int32, (1, WIDE), 1))
    down = canonical_rows(lax.broadcasted_iota(jnp.int32, (WIDE, 1), 0))
    for n, copy in enumerate(copies):
        for z in range(cz):
            line = order[n // cy, n % cy, z : z + 1, :].astype(f32)
            spread = jnp.broadcast_to(line, (128, PATCH)).T
            spread = jnp.concatenate([spread] * (WIDE // 128), axis=1)
            pick[n * cz + z] = jnp.where(spread == across, 1.0, 0.0).astype(bf16)
            back[n * cz + z] = jnp.where(down == line, 1.0, 0.0).astype(bf16)
        copy.wait()
        matrix[n] = loaded[n].reshape(cz * PATCH, PATCH)


def tables(cells, inverse, order):
    cx, cy, cz = cells
    count = cx * cy * cz
    vmem = pl.BlockSpec(memory_space=pltpu.VMEM)
    return pl.pallas_call(
        functools.partial(tables_kernel, cells),
        in_specs=[pl.BlockSpec(memory_space=pltpu.HBM), vmem],
        out_specs=[vmem] * 3,
        out_shape=[
            jax.ShapeDtypeStruct((cx * cy, cz * PATCH, PATCH), bf16),
            jax.ShapeDtypeStruct((count, PATCH, WIDE), bf16),
            jax.ShapeDtypeStruct((count, WIDE, PATCH), bf16),
        ],
        scratch_shapes=[
            pltpu.VMEM((cx * cy, PATCH, cz, PATCH), bf16),
            pltpu.SemaphoreType.DMA((cx * cy,)),
        ],
        compiler_params=pltpu.CompilerParams(vmem_limit_bytes=VMEM_LIMIT),
        cost_estimate=pl.CostEstimate(
            flops=count * 16 * WIDE * PATCH * 128,
            bytes_accessed=count * 2 * PATCH * PATCH,
            transcendentals=0,
        ),
        name="tables",
    )(inverse, order)


def exact_parts(value):
    high = value.astype(bf16)
    rest = value - high.astype(f32)
    middle = rest.astype(bf16)
    return high, middle, (rest - middle.astype(f32)).astype(bf16)


def matrices_kernel(depth, mat, slot, canon, both):
    both[...] = mat[0, 0].reshape(depth * LOCAL, LOCAL)
    index = lax.broadcasted_iota(jnp.int32, (LOCAL, LOCAL), 0)
    dims = (((1,), (1,)), ((), ()))
    for z in range(depth):
        pick = jnp.where(index == slot[z], 1.0, 0.0).astype(bf16)
        parts = exact_parts(both[pl.ds(z, LOCAL, stride=depth), :])
        side = sum(lax.dot_general(p, pick, dims, preferred_element_type=f32) for p in parts)
        parts = exact_parts(side)
        canon[z] = sum(jnp.dot(pick, p, preferred_element_type=f32) for p in parts)


def canonical_matrices(cells, matrices, face_order):
    cx, cy, cz = cells
    count = cx * cy * cz
    offsets = (INNER + FACE * jnp.arange(6, dtype=jnp.int32))[:, None]
    slots = (face_order + offsets).reshape(count, 1, 6 * FACE)
    inner = jnp.broadcast_to(jnp.arange(INNER, dtype=jnp.int32), (count, 1, INNER))
    slots = jnp.concatenate([inner, slots], axis=2)
    return pl.pallas_call(
        functools.partial(matrices_kernel, cz),
        grid=(cx * cy,),
        in_specs=[
            pl.BlockSpec((1, 1, LOCAL, cz, LOCAL), lambda i: (i // cy, i % cy, 0, 0, 0)),
            pl.BlockSpec((cz, 1, LOCAL), lambda i: (i, 0, 0)),
        ],
        out_specs=pl.BlockSpec((cz, LOCAL, LOCAL), lambda i: (i, 0, 0)),
        out_shape=jax.ShapeDtypeStruct((count, LOCAL, LOCAL), f32),
        scratch_shapes=[pltpu.VMEM((cz * LOCAL, LOCAL), f32)],
        compiler_params=pltpu.CompilerParams(vmem_limit_bytes=VMEM_LIMIT),
        cost_estimate=pl.CostEstimate(
            flops=count * 24 * LOCAL**3, bytes_accessed=count * 8 * LOCAL**2, transcendentals=0
        ),
        name="matrices",
    )(jnp.transpose(matrices, (0, 1, 3, 2, 4)), slots)


def call(kernel, operands, shapes, name):
    specs = [pl.BlockSpec(memory_space=pltpu.SMEM)]
    specs += [pl.BlockSpec(memory_space=pltpu.VMEM)] * (len(operands) - 1)
    return pl.pallas_call(
        kernel,
        in_specs=specs,
        out_specs=[pl.BlockSpec(memory_space=pltpu.VMEM)] * len(shapes),
        out_shape=[jax.ShapeDtypeStruct(s, t) for s, t in shapes],
        compiler_params=pltpu.CompilerParams(vmem_limit_bytes=VMEM_LIMIT),
        name=name,
    )(*operands)


def cat(*parts):
    return jnp.concatenate(parts, axis=0)


def zeros(rows, like):
    return jnp.zeros((rows, like.shape[-1]), f32)


def mixed(x, y, z, cells):
    return pl.ds((x * cells[1] + y) * OWN * cells[2] + z, OWN, stride=cells[2])


def start_kernel(cells, flags, res, out, my):
    cx, cy, cz = cells
    for x, y, z in itertools.product(*map(range, cells)):
        e = (x * cy + y) * cz + z
        cur = res[mixed(x, y, z, cells)]
        if y == 0:
            cur = cat(cur[:Y0], cur[Y0:Z0] * flags[0], cur[Z0:])
        if z == 0:
            cur = cat(cur[:Z0], cur[Z0:] * flags[2])
        out[e] = cur
        if y == cy - 1:
            nine, rest = zeros(FACE, cur), zeros(112 - OWN, cur)
            my[x * cz + z] = cat(cur[:Y0], nine, cur[Z0:], rest).astype(bf16)


def spread_kernel(cells, terms, *refs):
    cx, cy, cz = cells
    if terms:
        flags, res, yr, tx, tz, out, mx, mz, mxz = refs
    else:
        flags, res, yr, out, mx, mz, mxz = refs
    for x, z in itertools.product(range(cx), range(cz)):
        lastx, lastz = x == cx - 1, z == cz - 1
        halo = yr[0, x * cz + z].astype(f32) * flags[0]
        nine = zeros(FACE, halo)
        if lastx:
            mx[z] = cat(halo[:X0], halo[81:90], nine, halo[Z0:OWN]).astype(bf16)
        if lastz:
            mz[x * (cy + 1)] = cat(halo[:Y0], nine, halo[90:99]).astype(bf16)
        if lastx and lastz:
            mxz[0] = cat(halo[:X0], halo[81:90], nine, halo[90:99]).astype(bf16)
        for y in range(cy):
            e = (x * cy + y) * cz + z
            cur = res[e]
            if y == 0 and terms:
                cur = cat(cur[:Y0], cur[Y0:Z0] + halo[Y0:Z0], cur[Z0:])
            out[e] = cur
            upx = tx[y * cz + z][:FACE] if terms and lastx else nine
            upz = tz[x * cy + y][:FACE] if terms and lastz else nine
            if lastx:
                mx[(y + 1) * cz + z] = cat(cur[:X0], upx, cur[Y0:]).astype(bf16)
            if lastz:
                mz[x * (cy + 1) + y + 1] = cat(cur[:Z0], upz).astype(bf16)
            if lastx and lastz:
                mxz[y + 1] = cat(cur[:X0], upx, cur[Y0:Z0], upz).astype(bf16)


def solve_kernel(cells, *refs):
    flags, matrix, pick, back, res, yr, hx, hz, hxz = refs[:9]
    c, ox, oz, oxz, stars, solved, both = refs[9:]
    cx, cy, cz = cells
    columns = res.shape[-1]

    found = {}
    for e in itertools.product(range(-1, cx), range(-1, cy), range(-1, cz)):
        x, y, z = e
        if x < 0 and z < 0:
            val = hxz[y + 1].astype(f32) * flags[2]
        elif x < 0:
            val = hx[(y + 1) * cz + z].astype(f32)
        elif z < 0:
            val = hz[x * (cy + 1) + y + 1].astype(f32) * flags[2]
        elif y < 0:
            val = yr[0, x * cz + z].astype(f32)[:OWN] * flags[0]
        else:
            val = res[(x * cy + y) * cz + z]
        found[e] = val
    for n, v in enumerate(itertools.product(*map(range, cells))):
        for a, b, g in CORNERS:
            x, y, z = v[0] - 1 + a, v[1] - 1 + b, v[2] - 1 + g
            val = found[(x, y, z)]
            nine = zeros(FACE, val)
            part = cat(
                val[:X0],
                val[X0:Y0] if a or x < 0 else nine,
                val[Y0:Z0] if b else nine,
                val[Z0:] if g or z < 0 else nine,
                zeros(SLOT - OWN, val),
            )
            m = 4 * a + 2 * b + g
            stars[n, m * SLOT : (m + 1) * SLOT] = part.astype(bf16)

    @pl.loop(0, cx * cy)
    def _(step):
        listed = []
        for z in range(cz):
            n = step * cz + z
            got = jnp.dot(pick[n], stars[n], preferred_element_type=f32)
            listed.append(got.astype(bf16))
        listed = jnp.concatenate(listed, axis=1)
        answer = jnp.dot(matrix[step], listed, preferred_element_type=f32)
        for z in range(cz):
            both[z] = answer[:, z * columns : (z + 1) * columns]
        for z in range(cz):
            n = step * cz + z
            value = both[z, pl.ds(z, PATCH, stride=cz), :].astype(bf16)
            solved[n] = jnp.dot(back[n], value, preferred_element_type=f32)

    vertices = list(itertools.product(*map(range, cells)))
    for e in itertools.product(range(-1, cx), range(-1, cy), range(-1, cz)):
        parts = []
        for n, v in enumerate(vertices):
            m = tuple(e[d] - v[d] + 1 for d in range(3))
            if all(k in (0, 1) for k in m):
                parts.append((n, m))

        def total(low, high, keep):
            acc = None
            for n, m in parts:
                if keep(m):
                    base = (4 * m[0] + 2 * m[1] + m[2]) * SLOT
                    val = solved[n, base + low : base + high]
                    acc = val if acc is None else acc + val
            return acc

        pieces = [total(0, X0, lambda m: True)]
        for d in range(3):
            low = INNER + d * FACE
            pieces.append(total(low, low + FACE, lambda m: e[d] < 0 or m[d] == 1))
        val = cat(*pieces)
        x, y, z = e
        if x < 0 and z < 0:
            oxz[y + 1] = val.astype(bf16)
        elif x < 0:
            ox[(y + 1) * cz + z] = val.astype(bf16)
        elif z < 0:
            oz[x * (cy + 1) + y + 1] = val.astype(bf16)
        else:
            c[(x * (cy + 1) + y + 1) * cz + z] = val


def solve(cells, operands):
    cx, cy, cz = cells
    count, columns = cx * cy * cz, operands[4].shape[-1]
    vmem = pl.BlockSpec(memory_space=pltpu.VMEM)
    halos = operands[-3:]
    return pl.pallas_call(
        functools.partial(solve_kernel, cells),
        in_specs=[pl.BlockSpec(memory_space=pltpu.SMEM)] + [vmem] * (len(operands) - 1),
        out_specs=[vmem] * 4,
        out_shape=[jax.ShapeDtypeStruct((cx * (cy + 1) * cz, OWN, columns), f32)]
        + [jax.ShapeDtypeStruct(h.shape, bf16) for h in halos],
        scratch_shapes=[
            pltpu.VMEM((count, WIDE, columns), bf16),
            pltpu.VMEM((count, WIDE, columns), f32),
            pltpu.VMEM((cz, cz * PATCH, columns), f32),
        ],
        compiler_params=pltpu.CompilerParams(vmem_limit_bytes=VMEM_LIMIT),
        name="solve",
    )(*operands)


def add_received(val, x, y, z, cells, last, gx, gz, gxz):
    cx, cy, cz = cells
    nine = zeros(FACE, val)
    if x == cx - 1:
        got = gx[(y + 1) * cz + z].astype(f32)
        val = val + cat(got[:X0], nine, got[Y0:])
    if z == cz - 1:
        got = gz[x * (cy + 1) + y + 1].astype(f32) * last
        val = val + cat(got[:Z0], nine)
    if x == cx - 1 and z == cz - 1:
        got = gxz[y + 1].astype(f32) * last
        val = val + cat(got[:X0], nine, got[Y0:Z0], nine)
    return val


def upper_x(y, z, cells, last, gx, gxz):
    val = gx[(y + 1) * cells[2] + z].astype(f32)[X0:Y0]
    if z == cells[2] - 1:
        val = val + gxz[y + 1].astype(f32)[X0:Y0] * last
    return val


def upper_z(x, y, cells, last, gz, gxz):
    val = gz[x * (cells[1] + 1) + y + 1].astype(f32)[Z0:]
    if x == cells[0] - 1:
        val = val + gxz[y + 1].astype(f32)[Z0:]
    return val * last


def reduce_kernel(cells, flags, c, gx, gz, gxz, out):
    cx, cy, cz = cells
    for x, z in itertools.product(range(cx), range(cz)):
        val = add_received(c[x * (cy + 1) * cz + z], x, -1, z, cells, flags[3], gx, gz, gxz)
        nine = zeros(FACE, val)
        upx = upper_x(-1, z, cells, flags[3], gx, gxz) if x == cx - 1 else nine
        upz = upper_z(x, -1, cells, flags[3], gz, gxz) if z == cz - 1 else nine
        out[x * cz + z] = cat(val, upx, upz, zeros(104 - OWN - 2 * FACE, val))


def element_kernel(cells, first, last, *refs):
    cx, cy, cz = cells
    flags, c, gx, gz, gxz, yr, mat, res, hx, hz = refs[:10]
    refs = refs[10:]
    if not first:
        prev, refs = refs[0], refs[1:]
    sol, out, tx, tz, my = refs
    peer = yr.shape[0] - 1
    own, images = {}, {}
    for e in itertools.product(*map(range, cells)):
        x, y, z = e
        n = (x * cy + y) * cz + z
        val = add_received(c[(x * (cy + 1) + y + 1) * cz + z], x, y, z, cells, flags[3], gx, gz, gxz)
        if y == cy - 1:
            got = yr[peer, x * cz + z][:OWN] * flags[1]
            val = val + cat(got[:Y0], zeros(FACE, val), got[Z0:])
        if y == 0:
            val = cat(val[:Y0], val[Y0:Z0] * flags[0], val[Z0:])
        if z == 0:
            val = cat(val[:Z0], val[Z0:] * flags[2])
        own[e] = val
        total = val if first else prev[n] + val
        if last:
            sol[mixed(x, y, z, cells)] = total
        else:
            sol[n] = total
    for e in itertools.product(*map(range, cells)):
        x, y, z = e
        if x < cx - 1:
            upx = own[(x + 1, y, z)][X0:Y0]
        else:
            upx = upper_x(y, z, cells, flags[3], gx, gxz)
            if y == cy - 1:
                upx = upx + yr[peer, x * cz + z][81:90] * flags[1]
        if y < cy - 1:
            upy = own[(x, y + 1, z)][Y0:Z0]
        else:
            upy = yr[peer, x * cz + z][Y0:Z0] * flags[1]
        if z < cz - 1:
            upz = own[(x, y, z + 1)][Z0:]
        else:
            upz = upper_z(x, y, cells, flags[3], gz, gxz)
            if y == cy - 1:
                upz = upz + yr[peer, x * cz + z][90:99] * flags[1]
        val = own[e]
        local = cat(val[:Y0], upx, val[Y0:Z0], upy, val[Z0:], upz)
        images[e] = jnp.dot(
            mat[(x * cy + y) * cz + z],
            local,
            precision=lax.Precision.HIGHEST,
            preferred_element_type=f32,
        )
    for e in itertools.product(*map(range, cells)):
        x, y, z = e
        n = (x * cy + y) * cz + z
        old, image = res[n], images[e]
        lowx = old[X0:Y0] - image[54:63]
        lowy = old[Y0:Z0] - image[72:81]
        lowz = old[Z0:] - image[90:99]
        if x > 0:
            lowx = lowx - images[(x - 1, y, z)][63:72]
        else:
            lowx = lowx + hx[(y + 1) * cz + z].astype(f32)[X0:Y0]
        if y > 0:
            lowy = lowy - images[(x, y - 1, z)][81:90]
        else:
            lowy = lowy * flags[0]
        if z > 0:
            lowz = lowz - images[(x, y, z - 1)][99:108]
        else:
            lowz = (lowz + hz[x * (cy + 1) + y + 1].astype(f32)[Z0:]) * flags[2]
        val = cat(old[:X0] - image[:X0], lowx, lowy, lowz)
        out[n] = val
        nine, seven = zeros(FACE, val), zeros(16 - FACE, val)
        upx, upy, upz = -image[63:72], -image[81:90], -image[99:108]
        if x == cx - 1:
            tx[y * cz + z] = cat(upx, seven)
        if z == cz - 1:
            tz[x * cy + y] = cat(upz, seven)
        if y == cy - 1 and last:
            my[x * cz + z] = cat(upy, seven)
        elif y == cy - 1:
            my[x * cz + z] = cat(
                val[:Y0],
                upy,
                val[Z0:],
                upx if x == cx - 1 else nine,
                upz if z == cz - 1 else nine,
                zeros(112 - OWN - 2 * FACE, val),
            ).astype(bf16)


def finish_kernel(cells, flags, res, fx, fy, fz, out):
    cx, cy, cz = cells
    for x, y, z in itertools.product(*map(range, cells)):
        n = (x * cy + y) * cz + z
        cur = res[n]
        lowx, lowy, lowz = cur[X0:Y0], cur[Y0:Z0], cur[Z0:]
        if x == 0:
            lowx = lowx + fx[y * cz + z][:FACE]
        if y == 0:
            lowy = lowy + fy[0, x * cz + z][:FACE] * flags[0]
        if z == 0:
            lowz = lowz + fz[x * cy + y][:FACE] * flags[2]
        out[mixed(x, y, z, cells)] = cat(cur[:X0], lowx, lowy, lowz)


def route(offset):
    sizes = [lax.axis_size(a) for a in AXES]
    flat = lambda c: (c[0] * sizes[1] + c[1]) * sizes[2] + c[2]
    pairs = []
    for spot in itertools.product(*map(range, sizes)):
        aim = [s + o for s, o in zip(spot, offset)]
        aim[0] %= sizes[0]
        aim[2] %= sizes[2]
        if all(0 <= a < s for a, s in zip(aim, sizes)):
            pairs.append((flat(spot), flat(aim)))
    return pairs


def send_xz(mx, mz, mxz, sign):
    return (
        lax.ppermute(mx, AXES, route((sign, 0, 0))),
        lax.ppermute(mz, AXES, route((0, 0, sign))),
        lax.ppermute(mxz, AXES, route((sign, 0, sign))),
    )


def send_y(my, sign):
    if lax.axis_size("gy") == 2:
        return lax.all_gather(my, "gy")
    return lax.ppermute(my, AXES, route((0, sign, 0)))[None]


def body(residual_start, patch_inverse, patch_order, element_matrix, face_order):
    cells = cx, cy, cz = residual_start.shape[:3]
    if min(cells) < 2:
        raise ValueError(cells)
    columns = residual_start.shape[4]
    count = cx * cy * cz
    at_y, at_z = lax.axis_index("gy"), lax.axis_index("gz")
    flags = jnp.stack(
        [
            at_y > 0,
            at_y < lax.axis_size("gy") - 1,
            at_z > 0,
            at_z < lax.axis_size("gz") - 1,
        ]
    ).astype(f32)
    bind = lambda kernel, *extra: functools.partial(kernel, cells, *extra)
    state = ((count, OWN, columns), f32)
    sent = (
        (((cy + 1) * cz, OWN, columns), bf16),
        ((cx * (cy + 1), OWN, columns), bf16),
        ((cy + 1, OWN, columns), bf16),
    )
    term_x, term_y, term_z = (((n, 16, columns), f32) for n in (cy * cz, cx * cz, cx * cy))
    rim = ((cx * cz, 112, columns), bf16)

    swap = lambda a: jnp.transpose(a, (0, 1, 3, 2, 4))
    flat = ((count * OWN, columns), f32)
    start = swap(residual_start).reshape(count * OWN, columns)
    residual, my = call(bind(start_kernel), [flags, start], [state, rim], "start")
    inverse = swap(patch_inverse)
    inverse = pltpu.with_memory_space_constraint(swap(patch_inverse), pltpu.HBM)
    order = patch_order
    terms, solution = [], []
    for sweep in range(SWEEPS):
        first, last = sweep == 0, sweep == SWEEPS - 1
        yr = send_y(my, 1)
        residual, mx, mz, mxz = call(
            bind(spread_kernel, not first), [flags, residual, yr] + terms, [state, *sent], "spread"
        )
        order, mx, mz, mxz = lax.optimization_barrier((order, mx, mz, mxz))
        hx, hz, hxz = send_xz(mx, mz, mxz, 1)
        matrix, pick, place = tables(cells, inverse, order)
        c, ox, oz, oxz = solve(cells, [flags, matrix, pick, place, residual, yr, hx, hz, hxz])
        if first:
            face_order, ox = lax.optimization_barrier((face_order, ox))
            canon = canonical_matrices(cells, element_matrix, face_order)
        gx, gz, gxz = send_xz(ox, oz, oxz, -1)
        (down,) = call(
            bind(reduce_kernel), [flags, c, gx, gz, gxz], [((cx * cz, 104, columns), f32)], "reduce"
        )
        back = send_y(down, -1)
        total, residual, tx, tz, my = call(
            bind(element_kernel, first, last),
            [flags, c, gx, gz, gxz, back, canon, residual, hx, hz] + solution,
            [flat if last else state, state, term_x, term_z, term_y if last else rim],
            "element",
        )
        terms, solution = [tx, tz], [total]
    fx = lax.ppermute(tx, AXES, route((1, 0, 0)))
    fz = lax.ppermute(tz, AXES, route((0, 0, 1)))
    fy = send_y(my, 1)
    (residual,) = call(bind(finish_kernel), [flags, residual, fx, fy, fz], [flat], "finish")
    shape = (cx, cy, OWN, cz, columns)
    return swap(total.reshape(shape)), swap(residual.reshape(shape))


def solution(mesh):
    return jax.shard_map(
        body,
        mesh=mesh,
        in_specs=(
            P("gx", "gy", "gz", None, None),
            P("gx", "gy", "gz", None, None),
            P("gx", "gy", "gz", None),
            P("gx", "gy", "gz", None, None),
            P("gx", "gy", "gz", None, None),
        ),
        out_specs=(P("gx", "gy", "gz", None, None), P("gx", "gy", "gz", None, None)),
        check_vma=False,
    )
```

```python
import functools
import itertools

import jax
import jax.numpy as jnp
from jax import lax
from jax.experimental import pallas as pl
from jax.experimental.pallas import tpu as pltpu
from jax.sharding import PartitionSpec as P

INNER = 54
FACE = 9
OWN = INNER + 3 * FACE
LOCAL = INNER + 6 * FACE
SWEEPS = 2
PATCH = 540
SLOT = 96
WIDE = 8 * SLOT
AXES = ("gx", "gy", "gz")
CORNERS = tuple(itertools.product((0, 1), repeat=3))
X0, Y0, Z0 = INNER, INNER + FACE, INNER + 2 * FACE
f32, bf16 = jnp.float32, jnp.bfloat16
VMEM_LIMIT = 12 * 1024 * 1024


FACE_ROWS = (
    lambda a, b, g: 8 * INNER + FACE * (2 * b + g),
    lambda a, b, g: 8 * INNER + FACE * (4 + 2 * a + g),
    lambda a, b, g: 8 * INNER + FACE * (8 + 2 * a + b),
)


def canonical_rows(q):
    m = (q * 683) >> 16
    r = q - SLOT * m
    d = ((r - INNER) * 57) >> 9
    a, b, c = m >> 2, (m >> 1) & 1, m & 1
    face = jnp.where(d == 0, 2 * b + c, jnp.where(d == 1, 4 + 2 * a + c, 8 + 2 * a + b))
    on_face = 8 * INNER + FACE * face + r - INNER - FACE * d
    row = jnp.where(r < INNER, INNER * m + r, jnp.where(r < OWN, on_face, -1))
    return row.astype(f32)


def tables_kernel(cells, inv, order, matrix, pick, back, loaded, sems):
    cx, cy, cz = cells
    copies = [
        pltpu.make_async_copy(inv.at[n // cy, n % cy], loaded.at[n], sems.at[n])
        for n in range(cx * cy)
    ]
    for copy in copies:
        copy.start()
    across = canonical_rows(lax.broadcasted_iota(jnp.int32, (1, WIDE), 1))
    down = lax.broadcasted_iota(jnp.int32, (PATCH, PATCH), 0).astype(f32)
    for n, copy in enumerate(copies):
        for z in range(cz):
            line = order[n // cy, n % cy, z : z + 1, :].astype(f32)
            spread = jnp.broadcast_to(line, (128, PATCH)).T
            spread = jnp.concatenate([spread] * (WIDE // 128), axis=1)
            pick[n * cz + z] = jnp.where(spread == across, 1.0, 0.0).astype(bf16)
            back[n * cz + z] = jnp.where(down == line, 1.0, 0.0).astype(bf16)
        copy.wait()
        matrix[n] = loaded[n].reshape(cz * PATCH, PATCH)


def tables(cells, inverse, order):
    cx, cy, cz = cells
    count = cx * cy * cz
    vmem = pl.BlockSpec(memory_space=pltpu.VMEM)
    return pl.pallas_call(
        functools.partial(tables_kernel, cells),
        in_specs=[pl.BlockSpec(memory_space=pltpu.HBM), vmem],
        out_specs=[vmem] * 3,
        out_shape=[
            jax.ShapeDtypeStruct((cx * cy, cz * PATCH, PATCH), bf16),
            jax.ShapeDtypeStruct((count, PATCH, WIDE), bf16),
            jax.ShapeDtypeStruct((count, PATCH, PATCH), bf16),
        ],
        scratch_shapes=[
            pltpu.VMEM((cx * cy, PATCH, cz, PATCH), bf16),
            pltpu.SemaphoreType.DMA((cx * cy,)),
        ],
        compiler_params=pltpu.CompilerParams(vmem_limit_bytes=VMEM_LIMIT),
        cost_estimate=pl.CostEstimate(
            flops=count * 16 * WIDE * PATCH * 128,
            bytes_accessed=count * 2 * PATCH * PATCH,
            transcendentals=0,
        ),
        name="tables",
    )(inverse, order)


def exact_parts(value):
    high = value.astype(bf16)
    rest = value - high.astype(f32)
    middle = rest.astype(bf16)
    return high, middle, (rest - middle.astype(f32)).astype(bf16)


def matrices_kernel(depth, mat, slot, canon, both):
    both[...] = mat[0, 0].reshape(depth * LOCAL, LOCAL)
    index = lax.broadcasted_iota(jnp.int32, (LOCAL, LOCAL), 0)
    dims = (((1,), (1,)), ((), ()))
    for z in range(depth):
        pick = jnp.where(index == slot[z], 1.0, 0.0).astype(bf16)
        parts = exact_parts(both[pl.ds(z, LOCAL, stride=depth), :])
        side = sum(lax.dot_general(p, pick, dims, preferred_element_type=f32) for p in parts)
        parts = exact_parts(side)
        canon[z] = sum(jnp.dot(pick, p, preferred_element_type=f32) for p in parts)


def canonical_matrices(cells, matrices, face_order):
    cx, cy, cz = cells
    count = cx * cy * cz
    offsets = (INNER + FACE * jnp.arange(6, dtype=jnp.int32))[:, None]
    slots = (face_order + offsets).reshape(count, 1, 6 * FACE)
    inner = jnp.broadcast_to(jnp.arange(INNER, dtype=jnp.int32), (count, 1, INNER))
    slots = jnp.concatenate([inner, slots], axis=2)
    return pl.pallas_call(
        functools.partial(matrices_kernel, cz),
        grid=(cx * cy,),
        in_specs=[
            pl.BlockSpec((1, 1, LOCAL, cz, LOCAL), lambda i: (i // cy, i % cy, 0, 0, 0)),
            pl.BlockSpec((cz, 1, LOCAL), lambda i: (i, 0, 0)),
        ],
        out_specs=pl.BlockSpec((cz, LOCAL, LOCAL), lambda i: (i, 0, 0)),
        out_shape=jax.ShapeDtypeStruct((count, LOCAL, LOCAL), f32),
        scratch_shapes=[pltpu.VMEM((cz * LOCAL, LOCAL), f32)],
        compiler_params=pltpu.CompilerParams(vmem_limit_bytes=VMEM_LIMIT),
        cost_estimate=pl.CostEstimate(
            flops=count * 24 * LOCAL**3, bytes_accessed=count * 8 * LOCAL**2, transcendentals=0
        ),
        name="matrices",
    )(jnp.transpose(matrices, (0, 1, 3, 2, 4)), slots)


def call(kernel, operands, shapes, name):
    specs = [pl.BlockSpec(memory_space=pltpu.SMEM)]
    specs += [pl.BlockSpec(memory_space=pltpu.VMEM)] * (len(operands) - 1)
    return pl.pallas_call(
        kernel,
        in_specs=specs,
        out_specs=[pl.BlockSpec(memory_space=pltpu.VMEM)] * len(shapes),
        out_shape=[jax.ShapeDtypeStruct(s, t) for s, t in shapes],
        compiler_params=pltpu.CompilerParams(vmem_limit_bytes=VMEM_LIMIT),
        name=name,
    )(*operands)


def cat(*parts):
    return jnp.concatenate(parts, axis=0)


def zeros(rows, like):
    return jnp.zeros((rows, like.shape[-1]), f32)


def mixed(x, y, z, cells):
    return pl.ds((x * cells[1] + y) * OWN * cells[2] + z, OWN, stride=cells[2])


def start_kernel(cells, flags, res, out, my):
    cx, cy, cz = cells
    for x, y, z in itertools.product(*map(range, cells)):
        e = (x * cy + y) * cz + z
        cur = res[mixed(x, y, z, cells)]
        if y == 0:
            cur = cat(cur[:Y0], cur[Y0:Z0] * flags[0], cur[Z0:])
        if z == 0:
            cur = cat(cur[:Z0], cur[Z0:] * flags[2])
        out[e] = cur
        if y == cy - 1:
            nine, rest = zeros(FACE, cur), zeros(112 - OWN, cur)
            my[x * cz + z] = cat(cur[:Y0], nine, cur[Z0:], rest).astype(bf16)


def spread_kernel(cells, terms, *refs):
    cx, cy, cz = cells
    if terms:
        flags, res, yr, tx, tz, out, mx, mz, mxz = refs
    else:
        flags, res, yr, out, mx, mz, mxz = refs
    for x, z in itertools.product(range(cx), range(cz)):
        lastx, lastz = x == cx - 1, z == cz - 1
        halo = yr[0, x * cz + z].astype(f32) * flags[0]
        nine = zeros(FACE, halo)
        if lastx:
            mx[z] = cat(halo[:X0], halo[81:90], nine, halo[Z0:OWN]).astype(bf16)
        if lastz:
            mz[x * (cy + 1)] = cat(halo[:Y0], nine, halo[90:99]).astype(bf16)
        if lastx and lastz:
            mxz[0] = cat(halo[:X0], halo[81:90], nine, halo[90:99]).astype(bf16)
        for y in range(cy):
            e = (x * cy + y) * cz + z
            cur = res[e]
            if y == 0 and terms:
                cur = cat(cur[:Y0], cur[Y0:Z0] + halo[Y0:Z0], cur[Z0:])
            out[e] = cur
            upx = tx[y * cz + z][:FACE] if terms and lastx else nine
            upz = tz[x * cy + y][:FACE] if terms and lastz else nine
            if lastx:
                mx[(y + 1) * cz + z] = cat(cur[:X0], upx, cur[Y0:]).astype(bf16)
            if lastz:
                mz[x * (cy + 1) + y + 1] = cat(cur[:Z0], upz).astype(bf16)
            if lastx and lastz:
                mxz[y + 1] = cat(cur[:X0], upx, cur[Y0:Z0], upz).astype(bf16)


def solve_kernel(cells, *refs):
    flags, matrix, pick, back, res, yr, hx, hz, hxz = refs[:9]
    c, ox, oz, oxz, stars, solved, both = refs[9:]
    cx, cy, cz = cells
    columns = res.shape[-1]

    found = {}
    for e in itertools.product(range(-1, cx), range(-1, cy), range(-1, cz)):
        x, y, z = e
        if x < 0 and z < 0:
            val = hxz[y + 1].astype(f32) * flags[2]
        elif x < 0:
            val = hx[(y + 1) * cz + z].astype(f32)
        elif z < 0:
            val = hz[x * (cy + 1) + y + 1].astype(f32) * flags[2]
        elif y < 0:
            val = yr[0, x * cz + z].astype(f32)[:OWN] * flags[0]
        else:
            val = res[(x * cy + y) * cz + z]
        found[e] = val
    for n, v in enumerate(itertools.product(*map(range, cells))):
        for a, b, g in CORNERS:
            x, y, z = v[0] - 1 + a, v[1] - 1 + b, v[2] - 1 + g
            val = found[(x, y, z)]
            nine = zeros(FACE, val)
            part = cat(
                val[:X0],
                val[X0:Y0] if a or x < 0 else nine,
                val[Y0:Z0] if b else nine,
                val[Z0:] if g or z < 0 else nine,
                zeros(SLOT - OWN, val),
            )
            m = 4 * a + 2 * b + g
            stars[n, m * SLOT : (m + 1) * SLOT] = part.astype(bf16)

    listed = []
    for n in range(cx * cy * cz):
        got = jnp.dot(pick[n], stars[n], preferred_element_type=f32)
        listed.append(got.astype(bf16))
    for step in range(cx * cy):
        pair = jnp.concatenate(listed[step * cz : (step + 1) * cz], axis=1)
        answer = jnp.dot(matrix[step], pair, preferred_element_type=f32)
        for z in range(cz):
            both[step * cz + z] = answer[:, z * columns : (z + 1) * columns]
    for n in range(cx * cy * cz):
        value = both[n, pl.ds(n % cz, PATCH, stride=cz), :].astype(bf16)
        solved[n] = jnp.dot(back[n], value, preferred_element_type=f32)

    vertices = list(itertools.product(*map(range, cells)))
    for e in itertools.product(range(-1, cx), range(-1, cy), range(-1, cz)):
        parts = []
        for n, v in enumerate(vertices):
            m = tuple(e[d] - v[d] + 1 for d in range(3))
            if all(k in (0, 1) for k in m):
                parts.append((n, m))

        def total(rows, base, keep):
            acc = None
            for n, m in parts:
                if keep(m):
                    low = base(*m)
                    val = solved[n, low : low + rows]
                    acc = val if acc is None else acc + val
            return acc

        pieces = [total(INNER, lambda a, b, g: INNER * (4 * a + 2 * b + g), lambda m: True)]
        for d, base in enumerate(FACE_ROWS):
            pieces.append(total(FACE, base, lambda m: e[d] < 0 or m[d] == 1))
        val = cat(*pieces)
        x, y, z = e
        if x < 0 and z < 0:
            oxz[y + 1] = val.astype(bf16)
        elif x < 0:
            ox[(y + 1) * cz + z] = val.astype(bf16)
        elif z < 0:
            oz[x * (cy + 1) + y + 1] = val.astype(bf16)
        else:
            c[(x * (cy + 1) + y + 1) * cz + z] = val


def solve(cells, operands):
    cx, cy, cz = cells
    count, columns = cx * cy * cz, operands[4].shape[-1]
    vmem = pl.BlockSpec(memory_space=pltpu.VMEM)
    halos = operands[-3:]
    return pl.pallas_call(
        functools.partial(solve_kernel, cells),
        in_specs=[pl.BlockSpec(memory_space=pltpu.SMEM)] + [vmem] * (len(operands) - 1),
        out_specs=[vmem] * 4,
        out_shape=[jax.ShapeDtypeStruct((cx * (cy + 1) * cz, OWN, columns), f32)]
        + [jax.ShapeDtypeStruct(h.shape, bf16) for h in halos],
        scratch_shapes=[
            pltpu.VMEM((count, WIDE, columns), bf16),
            pltpu.VMEM((count, PATCH, columns), f32),
            pltpu.VMEM((count, cz * PATCH, columns), f32),
        ],
        compiler_params=pltpu.CompilerParams(vmem_limit_bytes=VMEM_LIMIT),
        name="solve",
    )(*operands)


def add_received(val, x, y, z, cells, last, gx, gz, gxz):
    cx, cy, cz = cells
    nine = zeros(FACE, val)
    if x == cx - 1:
        got = gx[(y + 1) * cz + z].astype(f32)
        val = val + cat(got[:X0], nine, got[Y0:])
    if z == cz - 1:
        got = gz[x * (cy + 1) + y + 1].astype(f32) * last
        val = val + cat(got[:Z0], nine)
    if x == cx - 1 and z == cz - 1:
        got = gxz[y + 1].astype(f32) * last
        val = val + cat(got[:X0], nine, got[Y0:Z0], nine)
    return val


def upper_x(y, z, cells, last, gx, gxz):
    val = gx[(y + 1) * cells[2] + z].astype(f32)[X0:Y0]
    if z == cells[2] - 1:
        val = val + gxz[y + 1].astype(f32)[X0:Y0] * last
    return val


def upper_z(x, y, cells, last, gz, gxz):
    val = gz[x * (cells[1] + 1) + y + 1].astype(f32)[Z0:]
    if x == cells[0] - 1:
        val = val + gxz[y + 1].astype(f32)[Z0:]
    return val * last


def reduce_kernel(cells, flags, c, gx, gz, gxz, out):
    cx, cy, cz = cells
    for x, z in itertools.product(range(cx), range(cz)):
        val = add_received(c[x * (cy + 1) * cz + z], x, -1, z, cells, flags[3], gx, gz, gxz)
        nine = zeros(FACE, val)
        upx = upper_x(-1, z, cells, flags[3], gx, gxz) if x == cx - 1 else nine
        upz = upper_z(x, -1, cells, flags[3], gz, gxz) if z == cz - 1 else nine
        out[x * cz + z] = cat(val, upx, upz, zeros(104 - OWN - 2 * FACE, val))


def element_kernel(cells, first, last, *refs):
    cx, cy, cz = cells
    flags, c, gx, gz, gxz, yr, mat, res, hx, hz = refs[:10]
    refs = refs[10:]
    if not first:
        prev, refs = refs[0], refs[1:]
    sol, out, tx, tz, my = refs
    peer = yr.shape[0] - 1
    own, images = {}, {}
    for e in itertools.product(*map(range, cells)):
        x, y, z = e
        n = (x * cy + y) * cz + z
        val = add_received(c[(x * (cy + 1) + y + 1) * cz + z], x, y, z, cells, flags[3], gx, gz, gxz)
        if y == cy - 1:
            got = yr[peer, x * cz + z][:OWN] * flags[1]
            val = val + cat(got[:Y0], zeros(FACE, val), got[Z0:])
        if y == 0:
            val = cat(val[:Y0], val[Y0:Z0] * flags[0], val[Z0:])
        if z == 0:
            val = cat(val[:Z0], val[Z0:] * flags[2])
        own[e] = val
        total = val if first else prev[n] + val
        if last:
            sol[mixed(x, y, z, cells)] = total
        else:
            sol[n] = total
    for e in itertools.product(*map(range, cells)):
        x, y, z = e
        if x < cx - 1:
            upx = own[(x + 1, y, z)][X0:Y0]
        else:
            upx = upper_x(y, z, cells, flags[3], gx, gxz)
            if y == cy - 1:
                upx = upx + yr[peer, x * cz + z][81:90] * flags[1]
        if y < cy - 1:
            upy = own[(x, y + 1, z)][Y0:Z0]
        else:
            upy = yr[peer, x * cz + z][Y0:Z0] * flags[1]
        if z < cz - 1:
            upz = own[(x, y, z + 1)][Z0:]
        else:
            upz = upper_z(x, y, cells, flags[3], gz, gxz)
            if y == cy - 1:
                upz = upz + yr[peer, x * cz + z][90:99] * flags[1]
        val = own[e]
        local = cat(val[:Y0], upx, val[Y0:Z0], upy, val[Z0:], upz)
        images[e] = jnp.dot(
            mat[(x * cy + y) * cz + z],
            local,
            precision=lax.Precision.HIGHEST,
            preferred_element_type=f32,
        )
    for e in itertools.product(*map(range, cells)):
        x, y, z = e
        n = (x * cy + y) * cz + z
        old, image = res[n], images[e]
        lowx = old[X0:Y0] - image[54:63]
        lowy = old[Y0:Z0] - image[72:81]
        lowz = old[Z0:] - image[90:99]
        if x > 0:
            lowx = lowx - images[(x - 1, y, z)][63:72]
        else:
            lowx = lowx + hx[(y + 1) * cz + z].astype(f32)[X0:Y0]
        if y > 0:
            lowy = lowy - images[(x, y - 1, z)][81:90]
        else:
            lowy = lowy * flags[0]
        if z > 0:
            lowz = lowz - images[(x, y, z - 1)][99:108]
        else:
            lowz = (lowz + hz[x * (cy + 1) + y + 1].astype(f32)[Z0:]) * flags[2]
        val = cat(old[:X0] - image[:X0], lowx, lowy, lowz)
        out[n] = val
        nine, seven = zeros(FACE, val), zeros(16 - FACE, val)
        upx, upy, upz = -image[63:72], -image[81:90], -image[99:108]
        if x == cx - 1:
            tx[y * cz + z] = cat(upx, seven)
        if z == cz - 1:
            tz[x * cy + y] = cat(upz, seven)
        if y == cy - 1 and last:
            my[x * cz + z] = cat(upy, seven)
        elif y == cy - 1:
            my[x * cz + z] = cat(
                val[:Y0],
                upy,
                val[Z0:],
                upx if x == cx - 1 else nine,
                upz if z == cz - 1 else nine,
                zeros(112 - OWN - 2 * FACE, val),
            ).astype(bf16)


def finish_kernel(cells, flags, res, fx, fy, fz, out):
    cx, cy, cz = cells
    for x, y, z in itertools.product(*map(range, cells)):
        n = (x * cy + y) * cz + z
        cur = res[n]
        lowx, lowy, lowz = cur[X0:Y0], cur[Y0:Z0], cur[Z0:]
        if x == 0:
            lowx = lowx + fx[y * cz + z][:FACE]
        if y == 0:
            lowy = lowy + fy[0, x * cz + z][:FACE] * flags[0]
        if z == 0:
            lowz = lowz + fz[x * cy + y][:FACE] * flags[2]
        out[mixed(x, y, z, cells)] = cat(cur[:X0], lowx, lowy, lowz)


def route(offset):
    sizes = [lax.axis_size(a) for a in AXES]
    flat = lambda c: (c[0] * sizes[1] + c[1]) * sizes[2] + c[2]
    pairs = []
    for spot in itertools.product(*map(range, sizes)):
        aim = [s + o for s, o in zip(spot, offset)]
        aim[0] %= sizes[0]
        aim[2] %= sizes[2]
        if all(0 <= a < s for a, s in zip(aim, sizes)):
            pairs.append((flat(spot), flat(aim)))
    return pairs


def send_xz(mx, mz, mxz, sign):
    return (
        lax.ppermute(mx, AXES, route((sign, 0, 0))),
        lax.ppermute(mz, AXES, route((0, 0, sign))),
        lax.ppermute(mxz, AXES, route((sign, 0, sign))),
    )


def send_y(my, sign):
    if lax.axis_size("gy") == 2:
        return lax.all_gather(my, "gy")
    return lax.ppermute(my, AXES, route((0, sign, 0)))[None]


def body(residual_start, patch_inverse, patch_order, element_matrix, face_order):
    cells = cx, cy, cz = residual_start.shape[:3]
    if min(cells) < 2:
        raise ValueError(cells)
    columns = residual_start.shape[4]
    count = cx * cy * cz
    at_y, at_z = lax.axis_index("gy"), lax.axis_index("gz")
    flags = jnp.stack(
        [
            at_y > 0,
            at_y < lax.axis_size("gy") - 1,
            at_z > 0,
            at_z < lax.axis_size("gz") - 1,
        ]
    ).astype(f32)
    bind = lambda kernel, *extra: functools.partial(kernel, cells, *extra)
    state = ((count, OWN, columns), f32)
    sent = (
        (((cy + 1) * cz, OWN, columns), bf16),
        ((cx * (cy + 1), OWN, columns), bf16),
        ((cy + 1, OWN, columns), bf16),
    )
    term_x, term_y, term_z = (((n, 16, columns), f32) for n in (cy * cz, cx * cz, cx * cy))
    rim = ((cx * cz, 112, columns), bf16)

    swap = lambda a: jnp.transpose(a, (0, 1, 3, 2, 4))
    flat = ((count * OWN, columns), f32)
    start = swap(residual_start).reshape(count * OWN, columns)
    residual, my = call(bind(start_kernel), [flags, start], [state, rim], "start")
    inverse = swap(patch_inverse)
    inverse = pltpu.with_memory_space_constraint(swap(patch_inverse), pltpu.HBM)
    order = patch_order
    terms, solution = [], []
    for sweep in range(SWEEPS):
        first, last = sweep == 0, sweep == SWEEPS - 1
        yr = send_y(my, 1)
        residual, mx, mz, mxz = call(
            bind(spread_kernel, not first), [flags, residual, yr] + terms, [state, *sent], "spread"
        )
        order, mx, mz, mxz = lax.optimization_barrier((order, mx, mz, mxz))
        hx, hz, hxz = send_xz(mx, mz, mxz, 1)
        matrix, pick, place = tables(cells, inverse, order)
        c, ox, oz, oxz = solve(cells, [flags, matrix, pick, place, residual, yr, hx, hz, hxz])
        if first:
            face_order, ox = lax.optimization_barrier((face_order, ox))
            canon = canonical_matrices(cells, element_matrix, face_order)
        gx, gz, gxz = send_xz(ox, oz, oxz, -1)
        (down,) = call(
            bind(reduce_kernel), [flags, c, gx, gz, gxz], [((cx * cz, 104, columns), f32)], "reduce"
        )
        back = send_y(down, -1)
        total, residual, tx, tz, my = call(
            bind(element_kernel, first, last),
            [flags, c, gx, gz, gxz, back, canon, residual, hx, hz] + solution,
            [flat if last else state, state, term_x, term_z, term_y if last else rim],
            "element",
        )
        terms, solution = [tx, tz], [total]
    fx = lax.ppermute(tx, AXES, route((1, 0, 0)))
    fz = lax.ppermute(tz, AXES, route((0, 0, 1)))
    fy = send_y(my, 1)
    (residual,) = call(bind(finish_kernel), [flags, residual, fx, fy, fz], [flat], "finish")
    shape = (cx, cy, OWN, cz, columns)
    return swap(total.reshape(shape)), swap(residual.reshape(shape))


def solution(mesh):
    return jax.shard_map(
        body,
        mesh=mesh,
        in_specs=(
            P("gx", "gy", "gz", None, None),
            P("gx", "gy", "gz", None, None),
            P("gx", "gy", "gz", None),
            P("gx", "gy", "gz", None, None),
            P("gx", "gy", "gz", None, None),
        ),
        out_specs=(P("gx", "gy", "gz", None, None), P("gx", "gy", "gz", None, None)),
        check_vma=False,
    )
```

```python
import functools
import itertools

import jax
import jax.numpy as jnp
from jax import lax
from jax.experimental import pallas as pl
from jax.experimental.pallas import tpu as pltpu
from jax.sharding import PartitionSpec as P

INNER = 54
FACE = 9
OWN = INNER + 3 * FACE
LOCAL = INNER + 6 * FACE
SWEEPS = 2
PATCH = 540
SLOT = 96
WIDE = 8 * SLOT
AXES = ("gx", "gy", "gz")
CORNERS = tuple(itertools.product((0, 1), repeat=3))
X0, Y0, Z0 = INNER, INNER + FACE, INNER + 2 * FACE
f32, bf16 = jnp.float32, jnp.bfloat16
VMEM_LIMIT = 12 * 1024 * 1024


FACE_ROWS = (
    lambda a, b, g: 8 * INNER + FACE * (2 * b + g),
    lambda a, b, g: 8 * INNER + FACE * (4 + 2 * a + g),
    lambda a, b, g: 8 * INNER + FACE * (8 + 2 * a + b),
)


def canonical_rows(q):
    m = (q * 683) >> 16
    r = q - SLOT * m
    d = ((r - INNER) * 57) >> 9
    a, b, c = m >> 2, (m >> 1) & 1, m & 1
    face = jnp.where(d == 0, 2 * b + c, jnp.where(d == 1, 4 + 2 * a + c, 8 + 2 * a + b))
    on_face = 8 * INNER + FACE * face + r - INNER - FACE * d
    row = jnp.where(r < INNER, INNER * m + r, jnp.where(r < OWN, on_face, -1))
    return row.astype(f32)


def tables_kernel(cells, inv, order, matrix, pick, back, loaded, sems):
    cx, cy, cz = cells
    copies = [
        pltpu.make_async_copy(inv.at[n // cy, n % cy], loaded.at[n], sems.at[n])
        for n in range(cx * cy)
    ]
    for copy in copies:
        copy.start()
    across = canonical_rows(lax.broadcasted_iota(jnp.int32, (1, WIDE), 1))
    down = lax.broadcasted_iota(jnp.int32, (PATCH, PATCH), 0).astype(f32)
    for n, copy in enumerate(copies):
        for z in range(cz):
            line = order[n // cy, n % cy, z : z + 1, :].astype(f32)
            spread = jnp.broadcast_to(line, (128, PATCH)).T
            spread = jnp.concatenate([spread] * (WIDE // 128), axis=1)
            pick[n * cz + z] = jnp.where(spread == across, 1.0, 0.0).astype(bf16)
            back[n * cz + z] = jnp.where(down == line, 1.0, 0.0).astype(bf16)
        copy.wait()
        matrix[n] = loaded[n].reshape(cz * PATCH, PATCH)


def tables(cells, inverse, order):
    cx, cy, cz = cells
    count = cx * cy * cz
    vmem = pl.BlockSpec(memory_space=pltpu.VMEM)
    return pl.pallas_call(
        functools.partial(tables_kernel, cells),
        in_specs=[pl.BlockSpec(memory_space=pltpu.HBM), vmem],
        out_specs=[vmem] * 3,
        out_shape=[
            jax.ShapeDtypeStruct((cx * cy, cz * PATCH, PATCH), bf16),
            jax.ShapeDtypeStruct((count, PATCH, WIDE), bf16),
            jax.ShapeDtypeStruct((count, PATCH, PATCH), bf16),
        ],
        scratch_shapes=[
            pltpu.VMEM((cx * cy, PATCH, cz, PATCH), bf16),
            pltpu.SemaphoreType.DMA((cx * cy,)),
        ],
        compiler_params=pltpu.CompilerParams(vmem_limit_bytes=VMEM_LIMIT),
        cost_estimate=pl.CostEstimate(
            flops=count * 16 * WIDE * PATCH * 128,
            bytes_accessed=count * 2 * PATCH * PATCH,
            transcendentals=0,
        ),
        name="tables",
    )(inverse, order)


def exact_parts(value):
    high = value.astype(bf16)
    rest = value - high.astype(f32)
    middle = rest.astype(bf16)
    return high, middle, (rest - middle.astype(f32)).astype(bf16)


def matrices_kernel(depth, mat, slot, canon, both):
    both[...] = mat[0, 0].reshape(depth * LOCAL, LOCAL)
    index = lax.broadcasted_iota(jnp.int32, (LOCAL, LOCAL), 0)
    dims = (((1,), (1,)), ((), ()))
    for z in range(depth):
        pick = jnp.where(index == slot[z], 1.0, 0.0).astype(bf16)
        parts = exact_parts(both[pl.ds(z, LOCAL, stride=depth), :])
        side = sum(lax.dot_general(p, pick, dims, preferred_element_type=f32) for p in parts)
        parts = exact_parts(side)
        canon[z] = sum(jnp.dot(pick, p, preferred_element_type=f32) for p in parts)


def canonical_matrices(cells, matrices, face_order):
    cx, cy, cz = cells
    count = cx * cy * cz
    offsets = (INNER + FACE * jnp.arange(6, dtype=jnp.int32))[:, None]
    slots = (face_order + offsets).reshape(count, 1, 6 * FACE)
    inner = jnp.broadcast_to(jnp.arange(INNER, dtype=jnp.int32), (count, 1, INNER))
    slots = jnp.concatenate([inner, slots], axis=2)
    return pl.pallas_call(
        functools.partial(matrices_kernel, cz),
        grid=(cx * cy,),
        in_specs=[
            pl.BlockSpec((1, 1, LOCAL, cz, LOCAL), lambda i: (i // cy, i % cy, 0, 0, 0)),
            pl.BlockSpec((cz, 1, LOCAL), lambda i: (i, 0, 0)),
        ],
        out_specs=pl.BlockSpec((cz, LOCAL, LOCAL), lambda i: (i, 0, 0)),
        out_shape=jax.ShapeDtypeStruct((count, LOCAL, LOCAL), f32),
        scratch_shapes=[pltpu.VMEM((cz * LOCAL, LOCAL), f32)],
        compiler_params=pltpu.CompilerParams(vmem_limit_bytes=VMEM_LIMIT),
        cost_estimate=pl.CostEstimate(
            flops=count * 24 * LOCAL**3, bytes_accessed=count * 8 * LOCAL**2, transcendentals=0
        ),
        name="matrices",
    )(jnp.transpose(matrices, (0, 1, 3, 2, 4)), slots)


def call(kernel, operands, shapes, name):
    specs = [pl.BlockSpec(memory_space=pltpu.SMEM)]
    specs += [pl.BlockSpec(memory_space=pltpu.VMEM)] * (len(operands) - 1)
    return pl.pallas_call(
        kernel,
        in_specs=specs,
        out_specs=[pl.BlockSpec(memory_space=pltpu.VMEM)] * len(shapes),
        out_shape=[jax.ShapeDtypeStruct(s, t) for s, t in shapes],
        compiler_params=pltpu.CompilerParams(vmem_limit_bytes=VMEM_LIMIT),
        name=name,
    )(*operands)


def cat(*parts):
    return jnp.concatenate(parts, axis=0)


def zeros(rows, like):
    return jnp.zeros((rows, like.shape[-1]), f32)


def mixed(x, y, z, cells):
    return pl.ds((x * cells[1] + y) * OWN * cells[2] + z, OWN, stride=cells[2])


def start_kernel(cells, flags, res, out, my):
    cx, cy, cz = cells
    for x, y, z in itertools.product(*map(range, cells)):
        e = (x * cy + y) * cz + z
        cur = res[mixed(x, y, z, cells)]
        if y == 0:
            cur = cat(cur[:Y0], cur[Y0:Z0] * flags[0], cur[Z0:])
        if z == 0:
            cur = cat(cur[:Z0], cur[Z0:] * flags[2])
        out[e] = cur
        if y == cy - 1:
            nine, rest = zeros(FACE, cur), zeros(112 - OWN, cur)
            my[x * cz + z] = cat(cur[:Y0], nine, cur[Z0:], rest).astype(bf16)


def spread_kernel(cells, terms, *refs):
    cx, cy, cz = cells
    if terms:
        flags, res, yr, tx, tz, out, mx, mz, mxz = refs
    else:
        flags, res, yr, out, mx, mz, mxz = refs
    for x, z in itertools.product(range(cx), range(cz)):
        lastx, lastz = x == cx - 1, z == cz - 1
        halo = yr[0, x * cz + z].astype(f32) * flags[0]
        nine = zeros(FACE, halo)
        if lastx:
            mx[z] = cat(halo[:X0], halo[81:90], nine, halo[Z0:OWN]).astype(bf16)
        if lastz:
            mz[x * (cy + 1)] = cat(halo[:Y0], nine, halo[90:99]).astype(bf16)
        if lastx and lastz:
            mxz[0] = cat(halo[:X0], halo[81:90], nine, halo[90:99]).astype(bf16)
        for y in range(cy):
            e = (x * cy + y) * cz + z
            cur = res[e]
            if y == 0 and terms:
                cur = cat(cur[:Y0], cur[Y0:Z0] + halo[Y0:Z0], cur[Z0:])
            out[e] = cur
            upx = tx[y * cz + z][:FACE] if terms and lastx else nine
            upz = tz[x * cy + y][:FACE] if terms and lastz else nine
            if lastx:
                mx[(y + 1) * cz + z] = cat(cur[:X0], upx, cur[Y0:]).astype(bf16)
            if lastz:
                mz[x * (cy + 1) + y + 1] = cat(cur[:Z0], upz).astype(bf16)
            if lastx and lastz:
                mxz[y + 1] = cat(cur[:X0], upx, cur[Y0:Z0], upz).astype(bf16)


def solve_kernel(cells, *refs):
    flags, matrix, pick, back, res, yr, hx, hz, hxz = refs[:9]
    c, ox, oz, oxz, stars, solved, both = refs[9:]
    cx, cy, cz = cells
    columns = res.shape[-1]

    found = {}
    for e in itertools.product(range(-1, cx), range(-1, cy), range(-1, cz)):
        x, y, z = e
        if x < 0 and z < 0:
            val = hxz[y + 1].astype(f32) * flags[2]
        elif x < 0:
            val = hx[(y + 1) * cz + z].astype(f32)
        elif z < 0:
            val = hz[x * (cy + 1) + y + 1].astype(f32) * flags[2]
        elif y < 0:
            val = yr[0, x * cz + z].astype(f32)[:OWN] * flags[0]
        else:
            val = res[(x * cy + y) * cz + z]
        found[e] = val
    for n, v in enumerate(itertools.product(*map(range, cells))):
        for a, b, g in CORNERS:
            x, y, z = v[0] - 1 + a, v[1] - 1 + b, v[2] - 1 + g
            val = found[(x, y, z)]
            nine = zeros(FACE, val)
            part = cat(
                val[:X0],
                val[X0:Y0] if a or x < 0 else nine,
                val[Y0:Z0] if b else nine,
                val[Z0:] if g or z < 0 else nine,
                zeros(SLOT - OWN, val),
            )
            m = 4 * a + 2 * b + g
            stars[n, m * SLOT : (m + 1) * SLOT] = part.astype(bf16)

    listed = []
    for n in range(cx * cy * cz):
        got = jnp.dot(pick[n], stars[n], preferred_element_type=f32)
        listed.append(got.astype(bf16))
    for step in range(cx * cy):
        pair = jnp.concatenate(listed[step * cz : (step + 1) * cz], axis=1)
        answer = jnp.dot(matrix[step], pair, preferred_element_type=f32)
        for z in range(cz):
            both[step * cz + z] = answer[:, z * columns : (z + 1) * columns]
    for n in range(cx * cy * cz):
        value = both[n, pl.ds(n % cz, PATCH, stride=cz), :].astype(bf16)
        solved[n] = jnp.dot(back[n], value, preferred_element_type=f32)

    vertices = list(itertools.product(*map(range, cells)))
    for e in itertools.product(range(-1, cx), range(-1, cy), range(-1, cz)):
        parts = []
        for n, v in enumerate(vertices):
            m = tuple(e[d] - v[d] + 1 for d in range(3))
            if all(k in (0, 1) for k in m):
                parts.append((n, m))

        def total(rows, base, keep):
            acc = None
            for n, m in parts:
                if keep(m):
                    low = base(*m)
                    val = solved[n, low : low + rows]
                    acc = val if acc is None else acc + val
            return acc

        pieces = [total(INNER, lambda a, b, g: INNER * (4 * a + 2 * b + g), lambda m: True)]
        for d, base in enumerate(FACE_ROWS):
            pieces.append(total(FACE, base, lambda m: e[d] < 0 or m[d] == 1))
        val = cat(*pieces)
        x, y, z = e
        if x < 0 and z < 0:
            oxz[y + 1] = val.astype(bf16)
        elif x < 0:
            ox[(y + 1) * cz + z] = val.astype(bf16)
        elif z < 0:
            oz[x * (cy + 1) + y + 1] = val.astype(bf16)
        else:
            c[(x * (cy + 1) + y + 1) * cz + z] = val


def solve(cells, operands):
    cx, cy, cz = cells
    count, columns = cx * cy * cz, operands[4].shape[-1]
    vmem = pl.BlockSpec(memory_space=pltpu.VMEM)
    halos = operands[-3:]
    return pl.pallas_call(
        functools.partial(solve_kernel, cells),
        in_specs=[pl.BlockSpec(memory_space=pltpu.SMEM)] + [vmem] * (len(operands) - 1),
        out_specs=[vmem] * 4,
        out_shape=[jax.ShapeDtypeStruct((cx * (cy + 1) * cz, OWN, columns), f32)]
        + [jax.ShapeDtypeStruct(h.shape, bf16) for h in halos],
        scratch_shapes=[
            pltpu.VMEM((count, WIDE, columns), bf16),
            pltpu.VMEM((count, PATCH, columns), f32),
            pltpu.VMEM((count, cz * PATCH, columns), f32),
        ],
        compiler_params=pltpu.CompilerParams(vmem_limit_bytes=VMEM_LIMIT),
        name="solve",
    )(*operands)


def add_received(val, x, y, z, cells, last, gx, gz, gxz):
    cx, cy, cz = cells
    nine = zeros(FACE, val)
    if x == cx - 1:
        got = gx[(y + 1) * cz + z].astype(f32)
        val = val + cat(got[:X0], nine, got[Y0:])
    if z == cz - 1:
        got = gz[x * (cy + 1) + y + 1].astype(f32) * last
        val = val + cat(got[:Z0], nine)
    if x == cx - 1 and z == cz - 1:
        got = gxz[y + 1].astype(f32) * last
        val = val + cat(got[:X0], nine, got[Y0:Z0], nine)
    return val


def upper_x(y, z, cells, last, gx, gxz):
    val = gx[(y + 1) * cells[2] + z].astype(f32)[X0:Y0]
    if z == cells[2] - 1:
        val = val + gxz[y + 1].astype(f32)[X0:Y0] * last
    return val


def upper_z(x, y, cells, last, gz, gxz):
    val = gz[x * (cells[1] + 1) + y + 1].astype(f32)[Z0:]
    if x == cells[0] - 1:
        val = val + gxz[y + 1].astype(f32)[Z0:]
    return val * last


def reduce_kernel(cells, flags, c, gx, gz, gxz, out):
    cx, cy, cz = cells
    for x, z in itertools.product(range(cx), range(cz)):
        val = add_received(c[x * (cy + 1) * cz + z], x, -1, z, cells, flags[3], gx, gz, gxz)
        nine = zeros(FACE, val)
        upx = upper_x(-1, z, cells, flags[3], gx, gxz) if x == cx - 1 else nine
        upz = upper_z(x, -1, cells, flags[3], gz, gxz) if z == cz - 1 else nine
        out[x * cz + z] = cat(val, upx, upz, zeros(104 - OWN - 2 * FACE, val))


def element_kernel(cells, first, last, *refs):
    cx, cy, cz = cells
    flags, c, gx, gz, gxz, yr, mat, res, hx, hz = refs[:10]
    refs = refs[10:]
    if not first:
        prev, refs = refs[0], refs[1:]
    sol, out, tx, tz, my = refs
    peer = yr.shape[0] - 1
    own, images = {}, {}
    for e in itertools.product(*map(range, cells)):
        x, y, z = e
        n = (x * cy + y) * cz + z
        val = add_received(c[(x * (cy + 1) + y + 1) * cz + z], x, y, z, cells, flags[3], gx, gz, gxz)
        if y == cy - 1:
            got = yr[peer, x * cz + z][:OWN] * flags[1]
            val = val + cat(got[:Y0], zeros(FACE, val), got[Z0:])
        if y == 0:
            val = cat(val[:Y0], val[Y0:Z0] * flags[0], val[Z0:])
        if z == 0:
            val = cat(val[:Z0], val[Z0:] * flags[2])
        own[e] = val
        total = val if first else prev[n] + val
        if last:
            sol[mixed(x, y, z, cells)] = total
        else:
            sol[n] = total
    for e in itertools.product(*map(range, cells)):
        x, y, z = e
        if x < cx - 1:
            upx = own[(x + 1, y, z)][X0:Y0]
        else:
            upx = upper_x(y, z, cells, flags[3], gx, gxz)
            if y == cy - 1:
                upx = upx + yr[peer, x * cz + z][81:90] * flags[1]
        if y < cy - 1:
            upy = own[(x, y + 1, z)][Y0:Z0]
        else:
            upy = yr[peer, x * cz + z][Y0:Z0] * flags[1]
        if z < cz - 1:
            upz = own[(x, y, z + 1)][Z0:]
        else:
            upz = upper_z(x, y, cells, flags[3], gz, gxz)
            if y == cy - 1:
                upz = upz + yr[peer, x * cz + z][90:99] * flags[1]
        val = own[e]
        local = cat(val[:Y0], upx, val[Y0:Z0], upy, val[Z0:], upz)
        high, low, _ = exact_parts(mat[(x * cy + y) * cz + z])
        top, rest, _ = exact_parts(local)
        image = jnp.dot(high, top, preferred_element_type=f32)
        image = image + jnp.dot(high, rest, preferred_element_type=f32)
        images[e] = image + jnp.dot(low, top, preferred_element_type=f32)
    for e in itertools.product(*map(range, cells)):
        x, y, z = e
        n = (x * cy + y) * cz + z
        old, image = res[n], images[e]
        lowx = old[X0:Y0] - image[54:63]
        lowy = old[Y0:Z0] - image[72:81]
        lowz = old[Z0:] - image[90:99]
        if x > 0:
            lowx = lowx - images[(x - 1, y, z)][63:72]
        else:
            lowx = lowx + hx[(y + 1) * cz + z].astype(f32)[X0:Y0]
        if y > 0:
            lowy = lowy - images[(x, y - 1, z)][81:90]
        else:
            lowy = lowy * flags[0]
        if z > 0:
            lowz = lowz - images[(x, y, z - 1)][99:108]
        else:
            lowz = (lowz + hz[x * (cy + 1) + y + 1].astype(f32)[Z0:]) * flags[2]
        val = cat(old[:X0] - image[:X0], lowx, lowy, lowz)
        out[n] = val
        nine, seven = zeros(FACE, val), zeros(16 - FACE, val)
        upx, upy, upz = -image[63:72], -image[81:90], -image[99:108]
        if x == cx - 1:
            tx[y * cz + z] = cat(upx, seven)
        if z == cz - 1:
            tz[x * cy + y] = cat(upz, seven)
        if y == cy - 1 and last:
            my[x * cz + z] = cat(upy, seven)
        elif y == cy - 1:
            my[x * cz + z] = cat(
                val[:Y0],
                upy,
                val[Z0:],
                upx if x == cx - 1 else nine,
                upz if z == cz - 1 else nine,
                zeros(112 - OWN - 2 * FACE, val),
            ).astype(bf16)


def finish_kernel(cells, flags, res, fx, fy, fz, out):
    cx, cy, cz = cells
    for x, y, z in itertools.product(*map(range, cells)):
        n = (x * cy + y) * cz + z
        cur = res[n]
        lowx, lowy, lowz = cur[X0:Y0], cur[Y0:Z0], cur[Z0:]
        if x == 0:
            lowx = lowx + fx[y * cz + z][:FACE]
        if y == 0:
            lowy = lowy + fy[0, x * cz + z][:FACE] * flags[0]
        if z == 0:
            lowz = lowz + fz[x * cy + y][:FACE] * flags[2]
        out[mixed(x, y, z, cells)] = cat(cur[:X0], lowx, lowy, lowz)


def route(offset):
    sizes = [lax.axis_size(a) for a in AXES]
    flat = lambda c: (c[0] * sizes[1] + c[1]) * sizes[2] + c[2]
    pairs = []
    for spot in itertools.product(*map(range, sizes)):
        aim = [s + o for s, o in zip(spot, offset)]
        aim[0] %= sizes[0]
        aim[2] %= sizes[2]
        if all(0 <= a < s for a, s in zip(aim, sizes)):
            pairs.append((flat(spot), flat(aim)))
    return pairs


def send_xz(mx, mz, mxz, sign):
    return (
        lax.ppermute(mx, AXES, route((sign, 0, 0))),
        lax.ppermute(mz, AXES, route((0, 0, sign))),
        lax.ppermute(mxz, AXES, route((sign, 0, sign))),
    )


def send_y(my, sign):
    if lax.axis_size("gy") == 2:
        return lax.all_gather(my, "gy")
    return lax.ppermute(my, AXES, route((0, sign, 0)))[None]


def body(residual_start, patch_inverse, patch_order, element_matrix, face_order):
    cells = cx, cy, cz = residual_start.shape[:3]
    if min(cells) < 2:
        raise ValueError(cells)
    columns = residual_start.shape[4]
    count = cx * cy * cz
    at_y, at_z = lax.axis_index("gy"), lax.axis_index("gz")
    flags = jnp.stack(
        [
            at_y > 0,
            at_y < lax.axis_size("gy") - 1,
            at_z > 0,
            at_z < lax.axis_size("gz") - 1,
        ]
    ).astype(f32)
    bind = lambda kernel, *extra: functools.partial(kernel, cells, *extra)
    state = ((count, OWN, columns), f32)
    sent = (
        (((cy + 1) * cz, OWN, columns), bf16),
        ((cx * (cy + 1), OWN, columns), bf16),
        ((cy + 1, OWN, columns), bf16),
    )
    term_x, term_y, term_z = (((n, 16, columns), f32) for n in (cy * cz, cx * cz, cx * cy))
    rim = ((cx * cz, 112, columns), bf16)

    swap = lambda a: jnp.transpose(a, (0, 1, 3, 2, 4))
    flat = ((count * OWN, columns), f32)
    start = swap(residual_start).reshape(count * OWN, columns)
    residual, my = call(bind(start_kernel), [flags, start], [state, rim], "start")
    inverse = swap(patch_inverse)
    inverse = pltpu.with_memory_space_constraint(swap(patch_inverse), pltpu.HBM)
    order = patch_order
    terms, solution = [], []
    for sweep in range(SWEEPS):
        first, last = sweep == 0, sweep == SWEEPS - 1
        yr = send_y(my, 1)
        residual, mx, mz, mxz = call(
            bind(spread_kernel, not first), [flags, residual, yr] + terms, [state, *sent], "spread"
        )
        order, mx, mz, mxz = lax.optimization_barrier((order, mx, mz, mxz))
        hx, hz, hxz = send_xz(mx, mz, mxz, 1)
        matrix, pick, place = tables(cells, inverse, order)
        c, ox, oz, oxz = solve(cells, [flags, matrix, pick, place, residual, yr, hx, hz, hxz])
        if first:
            face_order, ox = lax.optimization_barrier((face_order, ox))
            canon = canonical_matrices(cells, element_matrix, face_order)
        gx, gz, gxz = send_xz(ox, oz, oxz, -1)
        (down,) = call(
            bind(reduce_kernel), [flags, c, gx, gz, gxz], [((cx * cz, 104, columns), f32)], "reduce"
        )
        back = send_y(down, -1)
        total, residual, tx, tz, my = call(
            bind(element_kernel, first, last),
            [flags, c, gx, gz, gxz, back, canon, residual, hx, hz] + solution,
            [flat if last else state, state, term_x, term_z, term_y if last else rim],
            "element",
        )
        terms, solution = [tx, tz], [total]
    fx = lax.ppermute(tx, AXES, route((1, 0, 0)))
    fz = lax.ppermute(tz, AXES, route((0, 0, 1)))
    fy = send_y(my, 1)
    (residual,) = call(bind(finish_kernel), [flags, residual, fx, fy, fz], [flat], "finish")
    shape = (cx, cy, OWN, cz, columns)
    return swap(total.reshape(shape)), swap(residual.reshape(shape))


def solution(mesh):
    return jax.shard_map(
        body,
        mesh=mesh,
        in_specs=(
            P("gx", "gy", "gz", None, None),
            P("gx", "gy", "gz", None, None),
            P("gx", "gy", "gz", None),
            P("gx", "gy", "gz", None, None),
            P("gx", "gy", "gz", None, None),
        ),
        out_specs=(P("gx", "gy", "gz", None, None), P("gx", "gy", "gz", None, None)),
        check_vma=False,
    )
```
